32 devices in a mesh: grid: 32 (over z, y, x, core).
Axes of the slice: x: 2, y: 2, z: 4, core: 2. Of those that a mesh axis runs over, the one named last changes fastest.
Arguments:
- right_sides: float32 [32, 32, 48, 128], P(None, 'grid'), may hold values from -54 to 54, as said below
- recycle: float32 [2, 24, 32, 48, 128], P(None, None, 'grid'), may hold values from -6 to 6
- medium: float32 [32, 48, 128], P('grid'), may hold values from 0.05 to 1
- shift_table: float32 [8], replicated, may hold values from 0.25 to 2
- shift_index: int32 [2], replicated, may hold values from 0 to 7
Outputs:
- solution: float32 [32, 32, 48, 128], P(None, 'grid')
- residue: float32 [32, 32, 48, 128], P(None, 'grid')
The draws below stay inside these ranges and needn't reach their ends.
Inputs may be any that keep to these rules, and one draw needn't show every extreme that they name: `right_sides`: finite real values.
All inputs are finite; a program needn't handle non-finite values.
Results may differ from the reference program's by a relative error of at most 0.0003.
Values sent between devices are 32-bit elements; how exact they have to be, the bound alone decides.
A program may use at most 64 MiB of HBM per device.

```python
import math
import jax
import jax.numpy as jnp
from jax import lax

NX = 48
NY = 128
K = 24
B = 16
STEPS = 3
SHIFTS = 8
S = 32
NZ = 32


def draw_right_sides(key, part):
    keys = jax.random.split(key, 3)
    plane = jnp.exp(jax.random.uniform(keys[1], (NZ,), jnp.float32, math.log(0.3), math.log(3.0)))
    rising = 0.5 + jnp.arange(NZ, dtype=jnp.float32) / max(NZ - 1, 1)
    column = jnp.exp(jax.random.uniform(keys[2], (S,), jnp.float32, math.log(0.3), math.log(3.0)))
    rough = jnp.clip(jax.random.normal(keys[0], (S, NZ, NX, NY), jnp.float32), -4.0, 4.0)
    return rough * column[:, None, None, None] * (plane * rising)[None, :, None, None]


def level_of(rng, shape, shards, low, high):
    factor_of, own = 1.0, jax.random.fold_in(rng, 6)
    for axis_at, blocks in shards:
        heights = jnp.exp(jax.random.uniform(jax.random.fold_in(own, axis_at), (blocks,), jnp.float32, low / len(shards), high / len(shards)))
        factor_of = factor_of * jnp.repeat(heights, shape[axis_at] // blocks).reshape([-1 if axis == axis_at else 1 for axis in range(len(shape))])
    return factor_of


def gaussian(key, shape, scale, most, cuts=(), kind=jnp.bfloat16):
    entries = scale * jax.random.normal(key, shape, jnp.float32)
    if cuts:
        entries = entries * level_of(key, shape, cuts, -0.22, 0.18)
    return jnp.clip(entries, -most, most).astype(kind)


def setup_inputs(seed: int = 0) -> dict:
    key_of = jax.random.split(jax.random.key(seed), 6)
    return {
        "right_sides": draw_right_sides(jax.random.fold_in(key_of[5], 71), 0),
        "recycle": gaussian(key_of[1], (2, K, NZ, NX, NY), 1.0, 6.0, ((2, 32),), jnp.float32),
        "medium": jnp.clip(jnp.exp(math.log(1.0) - 2.9957323 * jax.random.uniform(key_of[2], (NZ, NX, NY), jnp.float32) ** level_of(key_of[2], (NZ, NX, NY), ((0, 32),), -0.2, 0.2)), 0.05, 1.0),
        "shift_table": jnp.clip(jnp.exp(jax.random.uniform(key_of[3], (SHIFTS,), jnp.float32, math.log(0.25), math.log(2.0))), 0.25, 2.0),
        "shift_index": jax.random.randint(key_of[4], (2,), 0, SHIFTS).astype(jnp.int32),
    }


highest = lax.Precision.HIGHEST

def operate(field, diagonal_field):
    padded = jnp.pad(field, ((0, 0), (1, 1), (1, 1), (1, 1)))
    beside = padded[:, 2:, 1:-1, 1:-1] + padded[:, :-2, 1:-1, 1:-1]
    beside = beside + padded[:, 1:-1, 2:, 1:-1] + padded[:, 1:-1, :-2, 1:-1]
    beside = beside + padded[:, 1:-1, 1:-1, 2:] + padded[:, 1:-1, 1:-1, :-2]
    return diagonal_field * field - beside

def flat_rows(field):
    return field.reshape(field.shape[0], -1)

def gram_of(left, right):
    return jnp.dot(left, right.T, precision=highest)

def combine(coeffs, vectors):
    return jnp.dot(coeffs, vectors, precision=highest)

def lower_solve(factor, values):
    return jax.scipy.linalg.solve_triangular(factor, values, lower=True)

def upper_solve(factor, values):
    return jax.scipy.linalg.solve_triangular(factor, values, lower=True, trans=1)

def least_squares(hessenberg, target):
    normal_factor = jnp.linalg.cholesky(jnp.dot(hessenberg.T, hessenberg, precision=highest))
    right_part = jnp.dot(hessenberg.T, target, precision=highest)
    return upper_solve(normal_factor, lower_solve(normal_factor, right_part))

def reference(right_sides, recycle, medium, shift_table, shift_index):
    field_shape = right_sides.shape[1:]
    solutions = []
    residues = []
    for member in range(2):
        diagonal_field = 6.0 + shift_table[shift_index[member]] + medium
        sources = flat_rows(right_sides[member * B:(member + 1) * B])
        basis_u = recycle[member]
        applied_u = flat_rows(operate(basis_u, diagonal_field))
        factor = jnp.linalg.cholesky(gram_of(applied_u, applied_u))
        projected = lower_solve(factor, gram_of(applied_u, sources))
        residual = sources - combine(upper_solve(factor, projected).T, applied_u)
        resid_factor = jnp.linalg.cholesky(gram_of(residual, residual))
        blocks = [lower_solve(resid_factor, residual)]
        hess_cols = []
        recycle_cols = []
        for number in range(STEPS):
            applied = flat_rows(operate(blocks[number].reshape((B,) + field_shape), diagonal_field))
            recycle_part = lower_solve(factor, gram_of(applied_u, applied))
            krylov_parts = [gram_of(block, applied) for block in blocks]
            applied = applied - combine(upper_solve(factor, recycle_part).T, applied_u)
            for block, part in zip(blocks, krylov_parts):
                applied = applied - combine(part.T, block)
            new_factor = jnp.linalg.cholesky(gram_of(applied, applied))
            hess_cols.append(jnp.concatenate(krylov_parts + [new_factor.T, jnp.zeros(((STEPS - 1 - number) * B, B), jnp.float32)], axis=0))
            recycle_cols.append(recycle_part)
            blocks.append(lower_solve(new_factor, applied))
        hessenberg = jnp.concatenate(hess_cols, axis=1)
        recycle_coef = jnp.concatenate(recycle_cols, axis=1)
        target = jnp.concatenate([resid_factor.T, jnp.zeros((STEPS * B, B), jnp.float32)], axis=0)
        minimizer = least_squares(hessenberg, target)
        back_coef = upper_solve(factor, projected - combine(recycle_coef, minimizer))
        krylov = jnp.concatenate(blocks[:STEPS], axis=0)
        solution = combine(minimizer.T, krylov) + combine(back_coef.T, flat_rows(basis_u))
        residue = combine((target - combine(hessenberg, minimizer)).T, jnp.concatenate(blocks, axis=0))
        solutions.append(solution.reshape((B,) + field_shape))
        residues.append(residue.reshape((B,) + field_shape))
    return (jnp.concatenate(solutions, axis=0), jnp.concatenate(residues, axis=0))
```

```python
import functools

import jax
import jax.numpy as jnp
from jax import lax
from jax.experimental import pallas as pl
from jax.experimental.pallas import tpu as pltpu
from jax.sharding import PartitionSpec as P

STEPS = 3
LANES = 128
MESH = pl.DeviceIdType.MESH
highest = lax.Precision.HIGHEST


def dot(left, right):
    return lax.dot_general(
        left, right, (((1,), (0,)), ((), ())), precision=highest, preferred_element_type=jnp.float32
    )


def dot_t(left, right):
    return lax.dot_general(
        left, right, (((1,), (1,)), ((), ())), precision=highest, preferred_element_type=jnp.float32
    )


def halves(x):
    high = x.astype(jnp.bfloat16)
    return high, (x - high.astype(jnp.float32)).astype(jnp.bfloat16)


def thirds(x):
    high, low = halves(x)
    return high, low, (x - high.astype(jnp.float32) - low.astype(jnp.float32)).astype(jnp.bfloat16)


def one(left, right):
    return jnp.dot(left, right, preferred_element_type=jnp.float32)


def one_t(left, right):
    return lax.dot_general(left, right, (((1,), (1,)), ((), ())), preferred_element_type=jnp.float32)


def iota2(shape, dim):
    return lax.broadcasted_iota(jnp.int32, shape, dim)


def eye(size):
    return jnp.where(iota2((size, size), 0) == iota2((size, size), 1), 1.0, 0.0)


def pair_step(arrays, k, first, second):
    c1, c2 = arrays[0][:, k : k + 1], arrays[0][:, k + 1 : k + 2]
    f1 = jnp.where(first, c1 * (1.0 / c1[k : k + 1]), 0.0)
    c2 = c2 - f1 * c2[k : k + 1]
    f2 = jnp.where(second, c2 * (1.0 / c2[k + 1 : k + 2]), 0.0)
    link = f1[k + 1 : k + 2]
    out = []
    for x in arrays:
        r1 = x[k : k + 1, :]
        r2 = x[k + 1 : k + 2, :] - link * r1
        out.append(x - f1 * r1 - f2 * r2)
    return tuple(out)


def factor(matrix, count):
    size = matrix.shape[0]
    rows = iota2((size, 1), 0)
    unit = jnp.where(rows < count, eye(size), 0.0)
    parts = (matrix, unit)
    for k in range(0, count, 2):
        parts = pair_step(parts, k, rows > k, rows > k + 1)
    a, z = parts
    upper = iota2((size, size), 1) >= iota2((size, size), 0)
    pivots = jnp.sum(a * unit, axis=1, keepdims=True)
    root = jnp.where(rows < count, lax.rsqrt(jnp.where(rows < count, pivots, 1.0)), 0.0)
    return jnp.where(upper, a * root, 0.0), z * root


def solve(matrix, right):
    size = matrix.shape[0]
    rows = iota2((size, 1), 0)
    parts = (matrix, right)
    for k in range(0, size, 2):
        parts = pair_step(parts, k, rows != k, rows != k + 1)
    a, r = parts
    return r / jnp.sum(a * eye(size), axis=1, keepdims=True)


def gray(j):
    return j + (j // 2) * (1 - 2 * lax.rem(j, 2))


def flip(t, d, bits):
    out = t
    for b in range(bits):
        out = out + (1 << b) * ((d >> b) & 1) * (1 - 2 * lax.rem(t // (1 << b), 2))
    return out


def kernel(
    n, quarters, stages,
    u_ref, b_ref, med_ref, table_ref, index_ref, sol_ref, res_ref,
    ubuf, vbuf, bbuf, mbuf, sh, sl, uh, ul, obuf, gram0, gram, coef, hbt, ebt, fin, back,
    in_send, in_recv, z_send, z_recv, x_send, x_recv, red_send, red_recv, out_send, out_recv,
):
    me = lax.axis_index("grid")
    planes = 2 * quarters
    bits = planes.bit_length() - 1
    k_rows = u_ref.shape[1]
    block = b_ref.shape[1]
    cells = b_ref.shape[2]
    ci = cells // quarters
    cw = ci + 2 * LANES
    tiles = ci // LANES
    pad = -(-k_rows // block) * block
    layers = n // planes
    lay, t = me // planes, lax.rem(me, planes)
    base = lay * planes
    core, q = lax.rem(t, 2), gray(t // 2)
    has_z = (lay > 0, lay < layers - 1)
    has_x = (q > 0, q < quarters - 1)
    z_to = (me - planes, me + planes)
    x_to = tuple(base + 2 * gray(q + s) + core for s in (-1, 1))

    barrier = pltpu.get_barrier_semaphore()
    peers = []
    for f, stride in stages:
        mine = lax.rem(me // stride, f)
        peers.append((f, stride, mine, me - mine * stride))
    greet = [base + flip(t, d, bits) for d in range(1, planes)]
    for f, stride, mine, first in peers:
        if stride >= planes:
            greet += [first + lax.rem(mine + d, f) * stride for d in range(1, f)]
    if layers > 1:
        greet += [lax.rem(me + planes, n), lax.rem(me + n - planes, n)]
    for to in greet:
        pl.semaphore_signal(barrier, inc=1, device_id=(to,), device_id_type=MESH)
    pl.semaphore_wait(barrier, len(greet))

    def part(qq, width):
        return pl.ds(pl.multiple_of(qq * ci, LANES), width)

    def in_copy(kind, there):
        to_core, to_q = lax.rem(there, 2), gray(there // 2)
        if kind == 0:
            src, dst = u_ref.at[to_core, :, part(to_q, cw)], ubuf.at[1 + t]
        elif kind == 1:
            src, dst = med_ref.at[:, part(to_q, ci)], mbuf.at[t]
        else:
            src, dst = b_ref.at[to_core, :, part(to_q, ci)], bbuf.at[t]
        return pltpu.make_async_remote_copy(
            src_ref=src, dst_ref=dst, send_sem=in_send.at[kind, there], recv_sem=in_recv.at[kind, t],
            device_id=(base + there,), device_id_type=MESH,
        )

    def in_wait(kind, there):
        dst = (ubuf.at[1 + there], mbuf.at[there], bbuf.at[there])[kind]
        pltpu.make_async_remote_copy(
            src_ref=dst, dst_ref=dst, send_sem=in_send.at[kind, there], recv_sem=in_recv.at[kind, there],
            device_id=(base + there,), device_id_type=MESH,
        ).wait_recv()

    others = [flip(t, d, bits) for d in range(planes - 1, 0, -1)]
    for kind in range(3):
        for there in others:
            in_copy(kind, there).start()
    ubuf[1 + t, :, :] = u_ref[core, :, part(q, cw)]
    mbuf[t, :, :] = med_ref[:, part(q, ci)]
    bbuf[t, :, :] = b_ref[core, :, part(q, ci)]

    shift = jnp.float32(0.0)
    for s in range(table_ref.shape[0]):
        shift = shift + jnp.where(index_ref[core] == s, table_ref[s], 0.0)
    shift = 6.0 + shift

    inner = pl.ds(LANES, ci)
    zero_plane = (0, planes + 1)
    for side in range(2):
        @pl.when(jnp.logical_not(has_z[side]))
        def _():
            ubuf[zero_plane[side]] = jnp.zeros(ubuf.shape[1:], jnp.float32)
            for j in range(STEPS):
                vbuf[j, zero_plane[side]] = jnp.zeros(vbuf.shape[2:], jnp.float32)

        @pl.when(jnp.logical_not(has_x[side]))
        def _():
            lanes = pl.ds((0, cw - LANES)[side], LANES)
            for j in range(STEPS):
                vbuf[j, :, :, lanes] = jnp.zeros((planes + 2, block, LANES), jnp.float32)

    def z_copy(stage, side):
        buf = ubuf if stage == 0 else vbuf.at[stage - 1]
        return pltpu.make_async_remote_copy(
            src_ref=buf.at[(1, planes)[side], :, inner], dst_ref=buf.at[(planes + 1, 0)[side], :, inner],
            send_sem=z_send.at[stage, side], recv_sem=z_recv.at[stage, side],
            device_id=(z_to[side],), device_id_type=MESH,
        )

    def x_copy(stage, side):
        buf = vbuf.at[stage - 1]
        mid = pl.ds(1, planes)
        return pltpu.make_async_remote_copy(
            src_ref=buf.at[mid, :, pl.ds((LANES, ci)[side], LANES)],
            dst_ref=buf.at[mid, :, pl.ds((cw - LANES, 0)[side], LANES)],
            send_sem=x_send.at[stage - 1, side], recv_sem=x_recv.at[stage - 1, side],
            device_id=(x_to[side],), device_id_type=MESH,
        )

    def both_sides(has, make, act):
        for side in range(2):
            @pl.when(has[side])
            def _():
                getattr(make(side), act)()

    def halo_start(has, make):
        both_sides(has, make, "start")

    def halo_wait(has, make):
        both_sides(has[::-1], make, "wait_recv")

    def reduce_sum(buffer, number, value):
        sem = number if buffer is gram0 else number + 1
        offset = 0
        for f, stride, mine, first in peers:
            own = offset + mine
            buffer[number, own, :, :] = value
            for d in range(1, f):
                to = lax.rem(mine + d, f)
                pltpu.make_async_remote_copy(
                    src_ref=buffer.at[number, own], dst_ref=buffer.at[number, own],
                    send_sem=red_send.at[sem, offset + d], recv_sem=red_recv.at[sem, own],
                    device_id=(first + to * stride,), device_id_type=MESH,
                ).start()
            for d in range(1, f):
                there = lax.rem(mine + d, f)
                origin = offset + there
                pltpu.make_async_remote_copy(
                    src_ref=buffer.at[number, origin], dst_ref=buffer.at[number, origin],
                    send_sem=red_send.at[sem, offset + d], recv_sem=red_recv.at[sem, origin],
                    device_id=(first + there * stride,), device_id_type=MESH,
                ).wait_recv()
            value = buffer[number, offset, :, :]
            for s in range(1, f):
                value = value + buffer[number, offset + s, :, :]
            offset += f
        return value

    def reduce_drain(buffer, number):
        sem = number if buffer is gram0 else number + 1
        offset = 0
        for f, stride, mine, first in peers:
            for d in range(1, f):
                pltpu.make_async_remote_copy(
                    src_ref=buffer.at[number, offset + mine], dst_ref=buffer.at[number, offset + mine],
                    send_sem=red_send.at[sem, offset + d], recv_sem=red_recv.at[sem, offset + mine],
                    device_id=(first + lax.rem(mine + d, f) * stride,), device_id_type=MESH,
                ).wait_send()
            offset += f

    lane = iota2((1, LANES), 1)

    def stencil(buf, p, tile):
        load = lambda z, s: buf[z, :, s * LANES : (s + 1) * LANES]
        c = load(p + 1, tile + 1)
        near = load(p + 1, tile) + load(p + 1, tile + 2)
        near = near + load(p, tile + 1) + load(p + 2, tile + 1)
        near = near + jnp.where(lane == 0, 0.0, pltpu.roll(c, 1, 1))
        near = near + jnp.where(lane == LANES - 1, 0.0, pltpu.roll(c, LANES - 1, 1))
        diag = mbuf[p, :, tile * LANES : (tile + 1) * LANES] + shift
        return diag * c - near, c

    def put(high, low, p, row, tile, value):
        at = slice(tile * LANES, (tile + 1) * LANES)
        h, l = halves(value)
        high[p, row : row + value.shape[0], at] = h
        low[p, row : row + value.shape[0], at] = l

    for kind in range(2):
        for there in others:
            in_wait(kind, there)
    halo_start(has_z, lambda side: z_copy(0, side))

    fill = jnp.zeros((pad - k_rows, LANES), jnp.float32)

    def widen(x):
        return jnp.concatenate([x, fill], axis=0) if pad > k_rows else x

    def image_plane(p, carry):
        for tile in range(tiles):
            applied, c = stencil(ubuf, p, tile)
            put(sh, sl, p, 0, tile, widen(applied))
            put(uh, ul, p, 0, tile, widen(c))
        return carry

    if planes > 2:
        lax.fori_loop(1, planes - 1, image_plane, 0)
    halo_wait(has_z, lambda side: z_copy(0, side))
    image_plane(0, 0)
    image_plane(planes - 1, 0)

    for there in others:
        in_wait(2, there)
    size = pad + block

    def first_gram(p, acc):
        for tile in range(tiles):
            put(sh, sl, p, pad, tile, bbuf[p, :, tile * LANES : (tile + 1) * LANES])
        rows = sh[p, 0:size, :]
        return acc + one_t(jnp.concatenate([rows, sl[p, 0:size, :]], axis=0), rows)

    acc = lax.fori_loop(0, planes, first_gram, jnp.zeros((2 * size, size), jnp.float32))
    cross = acc[size:, :]
    whole = acc[:size, :] + cross + dot_t(eye(size), cross)
    fin[0:k_rows, 0:size] = whole[0:k_rows, :]
    fin[0:k_rows, size:] = jnp.zeros((k_rows, LANES - size), jnp.float32)
    half = LANES // 2
    fin[0:block, half : half + block] = whole[pad:, pad:]
    fin[0:k_rows, :] = reduce_sum(gram0, 0, fin[0:k_rows, :])
    if pad > k_rows:
        fin[k_rows:pad, :] = jnp.zeros((pad - k_rows, LANES), jnp.float32)
    linv = factor(fin[0:pad, 0:pad], k_rows)[1]
    proj_t = dot_t(dot_t(eye(block), fin[0:pad, pad:size]), linv)
    remaining = fin[0:block, half : half + block] - dot_t(proj_t, proj_t)
    top_factor, inv = factor(remaining, block)
    coef[:, 0:pad] = -dot(inv, dot(proj_t, linv))
    coef[:, pad:size] = inv
    hbt[...] = jnp.zeros(hbt.shape, jnp.float32)

    unit = eye(block)
    for j in range(1, STEPS + 1):
        known = pad + block * j
        stacked = jnp.concatenate(thirds(coef[:, 0:known]), axis=0)

        def combine_plane(p, carry):
            first = one(stacked, sh[p, 0:known, :])
            second = one(stacked[0 : 2 * block], sl[p, 0:known, :])
            value = first[0:block] + (first[block : 2 * block] + second[0:block])
            value = value + (first[2 * block :] + second[block:])
            vbuf[j - 1, p + 1, :, inner] = value
            for tile in range(tiles):
                put(sh, sl, p, known - block, tile, value[:, tile * LANES : (tile + 1) * LANES])
            return carry

        combine_plane(0, 0)
        combine_plane(planes - 1, 0)
        halo_start(has_z, lambda side: z_copy(j, side))
        if planes > 2:
            lax.fori_loop(1, planes - 1, combine_plane, 0)
        halo_start(has_x, lambda side: x_copy(j, side))
        halo_wait(has_z, lambda side: z_copy(j, side))
        halo_wait(has_x, lambda side: x_copy(j, side))
        wide = known + block

        def gram_plane(p, acc):
            for tile in range(tiles):
                put(sh, sl, p, known, tile, stencil(vbuf.at[j - 1], p, tile)[0])
            rows, rest = sh[p, 0:wide, :], sl[p, 0:wide, :]
            new = jnp.concatenate([rows[known:], rest[known:]], axis=0)
            return acc + one_t(jnp.concatenate([rows, rest], axis=0), new)

        acc = lax.fori_loop(0, planes, gram_plane, jnp.zeros((2 * wide, 2 * block), jnp.float32))
        tall = acc[0:wide, 0:block] + (acc[wide:, 0:block] + acc[0:wide, block:] + acc[wide:, block:])
        fin[0:block, 0:wide] = dot_t(unit, tall)
        fin[0:block, :] = reduce_sum(gram, j - 1, fin[0:block, :])
        et = dot_t(fin[0:block, 0:pad], linv)
        ht = fin[0:block, pad:known]
        fresh = fin[0:block, known:wide] - dot_t(et, et) - dot_t(ht, ht)
        lt, inv = factor(fresh, block)
        coef[:, 0:pad] = -dot(inv, dot(et, linv))
        coef[:, pad:known] = -dot(inv, ht)
        coef[:, known:wide] = inv
        at = block * (j - 1)
        hbt[at : at + block, 0 : known - pad] = ht
        hbt[at : at + block, known - pad : known - pad + block] = dot_t(unit, lt)
        ebt[at : at + block, :] = et

    width = pad + block * (STEPS + 1)
    kry = block * STEPS
    h = hbt[:, 0 : kry + block]
    ys = solve(dot_t(h, h), dot(hbt[:, 0:block], top_factor))
    yt = dot_t(unit, ys)
    back[...] = dot(proj_t - dot(yt, ebt[...]), linv)
    fin[0:block, :] = -dot(yt, hbt[...])
    fin[0:block, 0:block] = fin[0:block, 0:block] + dot_t(unit, top_factor)
    top = fin[0:block, 0:kry]
    last = dot(fin[0:block, kry : kry + block], coef[:, 0:width])
    fin[...] = jnp.zeros(fin.shape, jnp.float32)
    fin[0:block, pad : pad + kry] = yt
    fin[block : 2 * block, 0:width] = last
    fin[block : 2 * block, pad : pad + kry] = fin[block : 2 * block, pad : pad + kry] + top
    high, low = halves(fin[0 : 2 * block, 0:width])
    stacked = jnp.concatenate([high, low], axis=0)
    bh, bl = halves(back[...])
    bstack = jnp.concatenate([bh, bl], axis=0)

    def out_copy(kind, there):
        dst = (sol_ref, res_ref)[kind]
        return pltpu.make_async_remote_copy(
            src_ref=obuf.at[there, pl.ds(kind * block, block)], dst_ref=dst.at[core, :, part(q, ci)],
            send_sem=out_send.at[kind, there], recv_sem=out_recv.at[kind, t],
            device_id=(base + there,), device_id_type=MESH,
        )

    def out_wait(kind, there):
        dst = (sol_ref, res_ref)[kind].at[lax.rem(there, 2), :, part(gray(there // 2), ci)]
        pltpu.make_async_remote_copy(
            src_ref=dst, dst_ref=dst, send_sem=out_send.at[kind, there], recv_sem=out_recv.at[kind, there],
            device_id=(base + there,), device_id_type=MESH,
        ).wait_recv()

    def final_plane(p):
        first = one(stacked, sh[p, 0:width, :])
        both = first[0 : 2 * block] + (first[2 * block :] + one(high, sl[p, 0:width, :]))
        first = one(bstack, uh[p])
        return both[0:block] + (first[0:block] + (first[block:] + one(bh, ul[p]))), both[block:]

    def final_send(i, carry):
        there = flip(t, planes - 1 - i, bits)
        sol, res = final_plane(there)
        obuf[there, 0:block, :] = sol
        obuf[there, block:, :] = res
        for kind in range(2):
            out_copy(kind, there).start()
        return carry

    lax.fori_loop(0, planes - 1, final_send, 0)
    sol, res = final_plane(t)
    sol_ref[core, :, part(q, ci)] = sol
    res_ref[core, :, part(q, ci)] = res

    for kind in range(3):
        for there in others:
            in_copy(kind, there).wait_send()
    for stage in range(STEPS + 1):
        both_sides(has_z, lambda side: z_copy(stage, side), "wait_send")
        if stage:
            both_sides(has_x, lambda side: x_copy(stage, side), "wait_send")
    reduce_drain(gram0, 0)
    for j in range(STEPS):
        reduce_drain(gram, j)
    for there in others:
        for kind in range(2):
            out_wait(kind, there)
            out_copy(kind, there).wait_send()


def split_count(n):
    out = []
    while n > 1:
        f = next(f for f in (4, 2, 8, n) if n % f == 0)
        out.append(f)
        n //= f
    return out


def solution(mesh):
    n = mesh.shape["grid"]

    def on_device(right_sides, recycle, medium, shift_table, shift_index):
        block = right_sides.shape[0] // 2
        k_rows = recycle.shape[1]
        lines = right_sides.shape[2]
        cells = lines * right_sides.shape[3]
        quarters = next(q for q in (4, 2, 1) if n % (2 * q) == 0 and lines % q == 0)
        planes = 2 * quarters
        stages, stride = [], 2
        for count in (quarters, n // planes):
            for f in split_count(count):
                stages.append((f, stride))
                stride *= f
        pad = -(-k_rows // block) * block
        ci = cells // quarters
        cw = ci + 2 * LANES
        width = pad + block * (STEPS + 1)
        b = right_sides.reshape(2, block, cells)
        u = jnp.pad(recycle.reshape(2, k_rows, cells), ((0, 0), (0, 0), (LANES, LANES)))
        slots = sum(f for f, _ in stages)
        vmem = pl.BlockSpec(memory_space=pltpu.VMEM)
        smem = pl.BlockSpec(memory_space=pltpu.SMEM)
        shape = jax.ShapeDtypeStruct((2, block, cells), jnp.float32)
        f32, half = jnp.float32, jnp.bfloat16
        sems = lambda *s: pltpu.SemaphoreType.DMA(s)
        sol, res = pl.pallas_call(
            functools.partial(kernel, n, quarters, tuple(stages)),
            out_shape=(shape, shape),
            in_specs=[vmem, vmem, vmem, smem, smem],
            out_specs=(vmem, vmem),
            scratch_shapes=[
                pltpu.VMEM((planes + 2, k_rows, cw), f32),
                pltpu.VMEM((STEPS, planes + 2, block, cw), f32),
                pltpu.VMEM((planes, block, ci), f32),
                pltpu.VMEM((planes, 1, ci), f32),
                pltpu.VMEM((planes, width, ci), half),
                pltpu.VMEM((planes, width, ci), half),
                pltpu.VMEM((planes, pad, ci), half),
                pltpu.VMEM((planes, pad, ci), half),
                pltpu.VMEM((planes, 2 * block, ci), f32),
                pltpu.VMEM((1, slots, k_rows, LANES), f32),
                pltpu.VMEM((STEPS, slots, block, LANES), f32),
                pltpu.VMEM((block, LANES), f32),
                pltpu.VMEM((block * STEPS, LANES), f32),
                pltpu.VMEM((block * STEPS, pad), f32),
                pltpu.VMEM((pad, LANES), f32),
                pltpu.VMEM((block, pad), f32),
                sems(3, planes), sems(3, planes),
                sems(STEPS + 1, 2), sems(STEPS + 1, 2),
                sems(STEPS, 2), sems(STEPS, 2),
                sems(STEPS + 1, slots), sems(STEPS + 1, slots),
                sems(2, planes), sems(2, planes),
            ],
            compiler_params=pltpu.CompilerParams(
                collective_id=0, has_side_effects=True, vmem_limit_bytes=48 * 1024 * 1024
            ),
        )(u, b, medium.reshape(1, cells), shift_table, shift_index)
        return sol.reshape(right_sides.shape), res.reshape(right_sides.shape)

    rows = P(None, "grid", None, None)
    return jax.shard_map(
        on_device,
        mesh=mesh,
        in_specs=(rows, P(None, None, "grid", None, None), P("grid", None, None), P(), P()),
        out_specs=(rows, rows),
        check_vma=False,
    )
```

```python
import functools

import jax
import jax.numpy as jnp
from jax import lax
from jax.experimental import pallas as pl
from jax.experimental.pallas import tpu as pltpu
from jax.sharding import PartitionSpec as P

STEPS = 3
LANES = 128
MESH = pl.DeviceIdType.MESH
highest = lax.Precision.HIGHEST


def dot(left, right):
    return lax.dot_general(
        left, right, (((1,), (0,)), ((), ())), precision=highest, preferred_element_type=jnp.float32
    )


def dot_t(left, right):
    return lax.dot_general(
        left, right, (((1,), (1,)), ((), ())), precision=highest, preferred_element_type=jnp.float32
    )


def halves(x):
    high = x.astype(jnp.bfloat16)
    return high, (x - high.astype(jnp.float32)).astype(jnp.bfloat16)


def thirds(x):
    high, low = halves(x)
    return high, low, (x - high.astype(jnp.float32) - low.astype(jnp.float32)).astype(jnp.bfloat16)


def one(left, right):
    return jnp.dot(left, right, preferred_element_type=jnp.float32)


def one_t(left, right):
    return lax.dot_general(left, right, (((1,), (1,)), ((), ())), preferred_element_type=jnp.float32)


def iota2(shape, dim):
    return lax.broadcasted_iota(jnp.int32, shape, dim)


def eye(size):
    return jnp.where(iota2((size, size), 0) == iota2((size, size), 1), 1.0, 0.0)


def pair_step(x, k, first, second):
    b1 = jnp.broadcast_to(x[:, k : k + 1], x.shape)
    b2 = jnp.broadcast_to(x[:, k + 1 : k + 2], x.shape)
    p12 = b2[k : k + 1]
    i1 = 1.0 / b1[k : k + 1]
    link = b1[k + 1 : k + 2] * i1
    i2 = 1.0 / (b2[k + 1 : k + 2] - link * p12)
    f1 = jnp.where(first, b1 * i1, 0.0)
    f2 = jnp.where(second, (b2 - f1 * p12) * i2, 0.0)
    r1 = x[k : k + 1, :]
    r2 = x[k + 1 : k + 2, :] - link * r1
    return x - f1 * r1 - f2 * r2


def beside(matrix, offset):
    size = matrix.shape[0]
    shape = (size, LANES)
    return jnp.where(iota2(shape, 1) == iota2(shape, 0) + offset, 1.0, matrix)


def factor(x, size, count):
    rows = iota2((size, 1), 0)
    diagonal = iota2((size, LANES), 1) == rows
    for k in range(0, count, 2):
        x = pair_step(x, k, rows > k, rows > k + 1)
    pivots = jnp.sum(jnp.where(diagonal, x, 0.0), axis=1, keepdims=True)
    root = jnp.where(rows < count, lax.rsqrt(jnp.where(rows < count, pivots, 1.0)), 0.0)
    x = x * root
    upper = iota2((size, size), 1) >= iota2((size, size), 0)
    return jnp.where(upper, x[:, 0:size], 0.0), x[:, size : 2 * size]


def eliminate(x, size):
    rows = iota2((size, 1), 0)
    for k in range(0, size, 2):
        x = pair_step(x, k, rows != k, rows != k + 1)
    diagonal = iota2((size, LANES), 1) == rows
    return x / jnp.sum(jnp.where(diagonal, x, 0.0), axis=1, keepdims=True)


def gray(j):
    return j + (j // 2) * (1 - 2 * lax.rem(j, 2))


def flip(t, d, bits):
    out = t
    for b in range(bits):
        out = out + (1 << b) * ((d >> b) & 1) * (1 - 2 * lax.rem(t // (1 << b), 2))
    return out


def kernel(
    n, quarters, stages,
    u_hbm, b_hbm, med_hbm, table_hbm, index_hbm, sol_lines, res_lines,
    u_lines, b_lines, med_ref, table_ref, index_ref,
    u_ref, b_ref, sol_ref, res_ref, ubuf, vbuf, bbuf, mbuf, sh, sl, uh, ul, obuf, gram0, gram, coef, hbt, ebt, lsq, fin, back,
    in_sem, in_send, in_recv, z_send, z_recv, x_send, x_recv, red_send, red_recv, out_send, out_recv,
):
    me = lax.axis_index("grid")
    planes = 2 * quarters
    bits = planes.bit_length() - 1
    takes = [
        pltpu.make_async_copy(src, dst, in_sem.at[i])
        for i, (src, dst) in enumerate((
            (u_hbm, u_lines), (b_hbm, b_lines), (med_hbm, med_ref), (table_hbm, table_ref), (index_hbm, index_ref)
        ))
    ]
    for take in takes:
        take.start()
    k_rows = u_ref.shape[1]
    block = b_ref.shape[1]
    cells = b_ref.shape[2]
    ci = cells // quarters
    cw = ci + 2 * LANES
    tiles = ci // LANES
    pad = -(-k_rows // block) * block
    layers = n // planes
    lay, t = me // planes, lax.rem(me, planes)
    base = lay * planes
    core, q = lax.rem(t, 2), gray(t // 2)
    has_z = (lay > 0, lay < layers - 1)
    has_x = (q > 0, q < quarters - 1)
    z_to = (me - planes, me + planes)
    x_to = tuple(base + 2 * gray(q + s) + core for s in (-1, 1))

    barrier = pltpu.get_barrier_semaphore()
    peers = []
    for f, stride in stages:
        mine = lax.rem(me // stride, f)
        peers.append((f, stride, mine, me - mine * stride))
    greet = [base + flip(t, d, bits) for d in range(1, planes)]
    for f, stride, mine, first in peers:
        greet += [first + lax.rem(mine + d, f) * stride for d in range(1, f)]
    if layers > 1:
        greet += [lax.rem(me + planes, n), lax.rem(me + n - planes, n)]
    for to in greet:
        pl.semaphore_signal(barrier, inc=1, device_id=(to,), device_id_type=MESH)

    lines = cells // LANES
    for g in range(2):
        u_ref[g, :, 0:LANES] = jnp.zeros((k_rows, LANES), jnp.float32)
        u_ref[g, :, cells + LANES :] = jnp.zeros((k_rows, LANES), jnp.float32)

    def take_u(x, carry):
        after = pl.ds(pl.multiple_of(x * LANES + LANES, LANES), LANES)
        for g in range(2):
            u_ref[g, :, after] = u_lines[g, :, x, :]
        return carry

    def take_b(x, carry):
        at = pl.ds(pl.multiple_of(x * LANES, LANES), LANES)
        for g in range(2):
            b_ref[g, :, at] = b_lines[g, :, x, :]
        return carry

    takes[0].wait()
    lax.fori_loop(0, lines, take_u, 0, unroll=4)
    for take in takes[1:]:
        take.wait()
    pl.semaphore_wait(barrier, len(greet))

    def part(qq, width):
        return pl.ds(pl.multiple_of(qq * ci, LANES), width)

    def in_copy(kind, there):
        to_core, to_q = lax.rem(there, 2), gray(there // 2)
        if kind == 0:
            src, dst = u_ref.at[to_core, :, part(to_q, cw)], ubuf.at[1 + t]
        elif kind == 1:
            src, dst = med_ref.at[:, part(to_q, ci)], mbuf.at[t]
        else:
            src, dst = b_ref.at[to_core, :, part(to_q, ci)], bbuf.at[t]
        return pltpu.make_async_remote_copy(
            src_ref=src, dst_ref=dst, send_sem=in_send.at[kind, there], recv_sem=in_recv.at[kind, t],
            device_id=(base + there,), device_id_type=MESH,
        )

    def in_wait(kind, there):
        dst = (ubuf.at[1 + there], mbuf.at[there], bbuf.at[there])[kind]
        pltpu.make_async_remote_copy(
            src_ref=dst, dst_ref=dst, send_sem=in_send.at[kind, there], recv_sem=in_recv.at[kind, there],
            device_id=(base + there,), device_id_type=MESH,
        ).wait_recv()

    others = [flip(t, d, bits) for d in range(planes - 1, 0, -1)]
    for kind in range(2):
        for there in others:
            in_copy(kind, there).start()

    lax.fori_loop(0, lines, take_b, 0, unroll=4)
    for there in others:
        in_copy(2, there).start()
    ubuf[1 + t, :, :] = u_ref[core, :, part(q, cw)]
    mbuf[t, :, :] = med_ref[:, part(q, ci)]
    bbuf[t, :, :] = b_ref[core, :, part(q, ci)]

    shift = jnp.float32(0.0)
    for s in range(table_ref.shape[0]):
        shift = shift + jnp.where(index_ref[core] == s, table_ref[s], 0.0)
    shift = 6.0 + shift

    inner = pl.ds(LANES, ci)
    zero_plane = (0, planes + 1)
    for side in range(2):
        @pl.when(jnp.logical_not(has_z[side]))
        def _():
            ubuf[zero_plane[side]] = jnp.zeros(ubuf.shape[1:], jnp.float32)
            for j in range(STEPS):
                vbuf[j, zero_plane[side]] = jnp.zeros(vbuf.shape[2:], jnp.float32)

        @pl.when(jnp.logical_not(has_x[side]))
        def _():
            lanes = pl.ds((0, cw - LANES)[side], LANES)
            for j in range(STEPS):
                vbuf[j, :, :, lanes] = jnp.zeros((planes + 2, block, LANES), jnp.float32)

    def z_copy(stage, side):
        buf = ubuf if stage == 0 else vbuf.at[stage - 1]
        return pltpu.make_async_remote_copy(
            src_ref=buf.at[(1, planes)[side], :, inner], dst_ref=buf.at[(planes + 1, 0)[side], :, inner],
            send_sem=z_send.at[stage, side], recv_sem=z_recv.at[stage, side],
            device_id=(z_to[side],), device_id_type=MESH,
        )

    def x_copy(stage, side):
        buf = vbuf.at[stage - 1]
        mid = pl.ds(1, planes)
        return pltpu.make_async_remote_copy(
            src_ref=buf.at[mid, :, pl.ds((LANES, ci)[side], LANES)],
            dst_ref=buf.at[mid, :, pl.ds((cw - LANES, 0)[side], LANES)],
            send_sem=x_send.at[stage - 1, side], recv_sem=x_recv.at[stage - 1, side],
            device_id=(x_to[side],), device_id_type=MESH,
        )

    def both_sides(has, make, act):
        for side in range(2):
            @pl.when(has[side])
            def _():
                getattr(make(side), act)()

    def halo_start(has, make):
        both_sides(has, make, "start")

    def halo_wait(has, make):
        both_sides(has[::-1], make, "wait_recv")

    def reduce_sum(buffer, number, value, meanwhile=None):
        sem = number if buffer is gram0 else number + 1
        offset = 0
        for f, stride, mine, first in peers:
            own = offset + mine
            buffer[number, own, :, :] = value
            for d in range(1, f):
                to = lax.rem(mine + d, f)
                pltpu.make_async_remote_copy(
                    src_ref=buffer.at[number, own], dst_ref=buffer.at[number, own],
                    send_sem=red_send.at[sem, offset + d], recv_sem=red_recv.at[sem, own],
                    device_id=(first + to * stride,), device_id_type=MESH,
                ).start()
            if meanwhile is not None:
                meanwhile()
                meanwhile = None
            for d in range(1, f):
                there = lax.rem(mine + d, f)
                origin = offset + there
                pltpu.make_async_remote_copy(
                    src_ref=buffer.at[number, origin], dst_ref=buffer.at[number, origin],
                    send_sem=red_send.at[sem, offset + d], recv_sem=red_recv.at[sem, origin],
                    device_id=(first + there * stride,), device_id_type=MESH,
                ).wait_recv()
            value = buffer[number, offset, :, :]
            for s in range(1, f):
                value = value + buffer[number, offset + s, :, :]
            offset += f
        return value

    def reduce_drain(buffer, number):
        sem = number if buffer is gram0 else number + 1
        offset = 0
        for f, stride, mine, first in peers:
            for d in range(1, f):
                pltpu.make_async_remote_copy(
                    src_ref=buffer.at[number, offset + mine], dst_ref=buffer.at[number, offset + mine],
                    send_sem=red_send.at[sem, offset + d], recv_sem=red_recv.at[sem, offset + mine],
                    device_id=(first + lax.rem(mine + d, f) * stride,), device_id_type=MESH,
                ).wait_send()
            offset += f

    lane = iota2((1, LANES), 1)

    def stencil(buf, p, tile):
        load = lambda z, s: buf[z, :, s * LANES : (s + 1) * LANES]
        c = load(p + 1, tile + 1)
        near = load(p + 1, tile) + load(p + 1, tile + 2)
        near = near + load(p, tile + 1) + load(p + 2, tile + 1)
        near = near + jnp.where(lane == 0, 0.0, pltpu.roll(c, 1, 1))
        near = near + jnp.where(lane == LANES - 1, 0.0, pltpu.roll(c, LANES - 1, 1))
        diag = mbuf[p, :, tile * LANES : (tile + 1) * LANES] + shift
        return diag * c - near, c

    def put(high, low, p, row, tile, value):
        at = slice(tile * LANES, (tile + 1) * LANES)
        h, l = halves(value)
        high[p, row : row + value.shape[0], at] = h
        low[p, row : row + value.shape[0], at] = l

    for kind in range(2):
        for there in others:
            in_wait(kind, there)
    halo_start(has_z, lambda side: z_copy(0, side))

    fill = jnp.zeros((pad - k_rows, LANES), jnp.float32)

    def widen(x):
        return jnp.concatenate([x, fill], axis=0) if pad > k_rows else x

    def image_plane(p, carry):
        for tile in range(tiles):
            applied, c = stencil(ubuf, p, tile)
            put(sh, sl, p, 0, tile, widen(applied))
            put(uh, ul, p, 0, tile, widen(c))
        return carry

    if planes > 2:
        lax.fori_loop(1, planes - 1, image_plane, 0)
    halo_wait(has_z, lambda side: z_copy(0, side))
    image_plane(0, 0)
    image_plane(planes - 1, 0)

    for there in others:
        in_wait(2, there)
    size = pad + block

    def first_gram(p, acc):
        for tile in range(tiles):
            put(sh, sl, p, pad, tile, bbuf[p, :, tile * LANES : (tile + 1) * LANES])
        rows = sh[p, 0:size, :]
        return acc + one_t(jnp.concatenate([rows, sl[p, 0:size, :]], axis=0), rows)

    acc = lax.fori_loop(0, planes, first_gram, jnp.zeros((2 * size, size), jnp.float32), unroll=min(4, planes))
    cross = acc[size:, :]
    whole = acc[:size, :] + cross + dot_t(eye(size), cross)
    fin[0:k_rows, 0:size] = whole[0:k_rows, :]
    fin[0:k_rows, size:] = jnp.zeros((k_rows, LANES - size), jnp.float32)
    half = LANES // 2
    fin[0:block, half : half + block] = whole[pad:, pad:]

    def clear():
        hbt[...] = jnp.zeros(hbt.shape, jnp.float32)
        lsq[...] = jnp.zeros(lsq.shape, jnp.float32)

    fin[0:k_rows, :] = reduce_sum(gram0, 0, fin[0:k_rows, :], clear)
    if pad > k_rows:
        fin[k_rows:pad, :] = jnp.zeros((pad - k_rows, LANES), jnp.float32)
    lanes = iota2((pad, LANES), 1)
    mixed = fin[0:pad, 0:size]
    linv = factor(beside(jnp.where(lanes < pad, fin[0:pad, :], 0.0), pad), pad, k_rows)[1]
    whole_inv = lax.dot_general(
        linv, linv, (((0,), (0,)), ((), ())), precision=highest, preferred_element_type=jnp.float32
    )
    ba = dot_t(eye(block), mixed[:, pad:size])
    ba_inv = dot(ba, whole_inv)
    remaining = fin[0:block, half : half + block] - dot_t(ba_inv, ba)
    wide_zero = jnp.zeros((block, LANES - block), jnp.float32)
    full = lambda m: jnp.concatenate([m, wide_zero], axis=1)
    top_factor, inv = factor(beside(full(remaining), block), block, block)
    coef[:, 0:pad] = -dot(inv, ba_inv)
    coef[:, pad:size] = inv

    unit = eye(block)
    lower = dot_t(unit, top_factor)
    for j in range(1, STEPS + 1):
        known = pad + block * j
        stacked = jnp.concatenate(thirds(coef[:, 0:known]), axis=0)

        def combine(p, first_tile, last_tile):
            at = slice(first_tile * LANES, last_tile * LANES)
            first = one(stacked, sh[p, 0:known, at])
            second = one(stacked[0 : 2 * block], sl[p, 0:known, at])
            value = first[0:block] + (first[block : 2 * block] + second[0:block])
            value = value + (first[2 * block :] + second[block:])
            vbuf[j - 1, p + 1, :, LANES + first_tile * LANES : LANES + last_tile * LANES] = value
            for tile in range(first_tile, last_tile):
                here = slice((tile - first_tile) * LANES, (tile - first_tile + 1) * LANES)
                put(sh, sl, p, known - block, tile, value[:, here])

        def combine_edges(p, carry):
            combine(p, 0, 1)
            combine(p, tiles - 1, tiles)
            return carry

        def combine_inner(p, carry):
            combine(p, 1, tiles - 1)
            return carry

        def image_inner(p, carry):
            for tile in range(1, tiles - 1):
                put(sh, sl, p, known, tile, stencil(vbuf.at[j - 1], p, tile)[0])
            return carry

        wide = known + block
        ends = (0, planes - 1)
        acc = jnp.zeros((2 * wide, 2 * block), jnp.float32)

        def gram_of(rows, rest):
            new = jnp.concatenate([rows[known:], rest[known:]], axis=0)
            return one_t(jnp.concatenate([rows, rest], axis=0), new)

        def image(p, tile):
            put(sh, sl, p, known, tile, stencil(vbuf.at[j - 1], p, tile)[0])

        def inner_gram(p, acc):
            for tile in range(1, tiles - 1):
                image(p, tile)
            at = slice(LANES, (tiles - 1) * LANES)
            return acc + gram_of(sh[p, 0:wide, at], sl[p, 0:wide, at])

        for p in ends:
            combine(p, 0, tiles)
        halo_start(has_z, lambda side: z_copy(j, side))
        for p in range(1, planes - 1):
            combine(p, 0, 1)
            combine(p, tiles - 1, tiles)
        halo_start(has_x, lambda side: x_copy(j, side))
        for p in range(1, planes - 1):
            combine(p, 1, tiles - 1)
        if planes > 2:
            acc = lax.fori_loop(1, planes - 1, inner_gram, acc, unroll=(planes - 2) // 2)
        halo_wait(has_x, lambda side: x_copy(j, side))
        lanes_of = lambda ref, p, tile: ref[p, 0:wide, tile * LANES : (tile + 1) * LANES]
        sides = [(p, tile) for p in range(1, planes - 1) for tile in (0, tiles - 1)]
        for p, tile in sides:
            image(p, tile)
        if sides:
            acc = acc + gram_of(*(
                jnp.concatenate([lanes_of(ref, p, tile) for p, tile in sides], axis=1) for ref in (sh, sl)
            ))
        halo_wait(has_z, lambda side: z_copy(j, side))
        for p in ends:
            for tile in range(tiles):
                image(p, tile)
            acc = acc + gram_of(sh[p, 0:wide, :], sl[p, 0:wide, :])
        tall = acc[0:wide, 0:block] + (acc[wide:, 0:block] + acc[0:wide, block:] + acc[wide:, block:])
        fin[0:block, 0:wide] = dot_t(unit, tall)
        early = block * (STEPS - 1)

        if j == STEPS:
            pads = jnp.zeros((early, LANES - early), jnp.float32)

            def invert_early():
                he = hbt[0:early, :]
                normal = jnp.concatenate([dot_t(he, he), pads], axis=1)
                lsq[...] = eliminate(beside(normal, early), early)

            fin[0:block, :] = reduce_sum(gram, j - 1, fin[0:block, :], invert_early)
        else:
            fin[0:block, :] = reduce_sum(gram, j - 1, fin[0:block, :])
        wa = fin[0:block, 0:pad]
        wa_inv = dot(wa, whole_inv)
        ht = fin[0:block, pad:known]
        fresh = fin[0:block, known:wide] - dot_t(ht, ht) - dot_t(wa_inv, wa)
        lt, inv = factor(beside(full(fresh), block), block, block)
        coef[:, 0:pad] = -dot(inv, wa_inv)
        coef[:, pad:known] = -dot(inv, ht)
        coef[:, known:wide] = inv
        at = block * (j - 1)
        hbt[at : at + block, 0 : known - pad] = ht
        hbt[at : at + block, known - pad : known - pad + block] = dot_t(unit, lt)
        ebt[at : at + block, :] = wa_inv

    width = pad + block * (STEPS + 1)
    kry = block * STEPS
    he, hl = hbt[0:early, :], hbt[early:kry, :]
    p = lsq[:, early : 2 * early]
    rt_early = dot_t(lower, he[:, 0:block])
    rt_late = dot_t(lower, hl[:, 0:block])
    cross = dot_t(hl, he)
    bent = dot(cross, p)
    schur = dot_t(hl, hl) - dot_t(bent, cross)
    yt0 = dot(rt_early, p)
    late_right = rt_late - dot_t(yt0, cross)
    both = jnp.concatenate([schur, dot_t(unit, late_right), wide_zero[:, block:]], axis=1)
    y_late = dot_t(unit, eliminate(both, block)[:, block : 2 * block])
    yt = jnp.concatenate([yt0 - dot(y_late, bent), y_late], axis=1)
    back[...] = ba_inv - dot(yt, ebt[...])
    fin[0:block, :] = -dot(yt, hbt[...])
    fin[0:block, 0:block] = fin[0:block, 0:block] + lower
    top = fin[0:block, 0:kry]
    last = dot(fin[0:block, kry : kry + block], coef[:, 0:width])
    fin[...] = jnp.zeros(fin.shape, jnp.float32)
    fin[0:block, pad : pad + kry] = yt
    fin[block : 2 * block, 0:width] = last
    fin[block : 2 * block, pad : pad + kry] = fin[block : 2 * block, pad : pad + kry] + top
    high, low = halves(fin[0 : 2 * block, 0:width])
    stacked = jnp.concatenate([high, low], axis=0)
    bh, bl = halves(back[...])
    bstack = jnp.concatenate([bh, bl], axis=0)

    def out_copy(kind, there):
        dst = (sol_ref, res_ref)[kind]
        return pltpu.make_async_remote_copy(
            src_ref=obuf.at[there, pl.ds(kind * block, block)], dst_ref=dst.at[core, :, part(q, ci)],
            send_sem=out_send.at[kind, there], recv_sem=out_recv.at[kind, t],
            device_id=(base + there,), device_id_type=MESH,
        )

    def out_wait(kind, there):
        dst = (sol_ref, res_ref)[kind].at[lax.rem(there, 2), :, part(gray(there // 2), ci)]
        pltpu.make_async_remote_copy(
            src_ref=dst, dst_ref=dst, send_sem=out_send.at[kind, there], recv_sem=out_recv.at[kind, there],
            device_id=(base + there,), device_id_type=MESH,
        ).wait_recv()

    def final_plane(p):
        first = one(stacked, sh[p, 0:width, :])
        both = first[0 : 2 * block] + (first[2 * block :] + one(high, sl[p, 0:width, :]))
        first = one(bstack, uh[p])
        return both[0:block] + (first[0:block] + (first[block:] + one(bh, ul[p]))), both[block:]

    def final_send(i, carry):
        there = flip(t, planes - 1 - i, bits)
        sol, res = final_plane(there)
        obuf[there, 0:block, :] = sol
        obuf[there, block:, :] = res
        for kind in range(2):
            out_copy(kind, there).start()
        return carry

    lax.fori_loop(0, planes - 1, final_send, 0)
    sol, res = final_plane(t)
    for x in range(tiles):
        sol_lines[core, :, q * tiles + x, :] = sol[:, x * LANES : (x + 1) * LANES]
        res_lines[core, :, q * tiles + x, :] = res[:, x * LANES : (x + 1) * LANES]

    for there in others:
        g, first_line = lax.rem(there, 2), gray(there // 2) * tiles
        for kind in range(2):
            out_wait(kind, there)
            landed, lines_of = (sol_ref, sol_lines, res_ref, res_lines)[2 * kind : 2 * kind + 2]
            for x in range(tiles):
                at = pl.ds(pl.multiple_of((first_line + x) * LANES, LANES), LANES)
                lines_of[g, :, first_line + x, :] = landed[g, :, at]
    for kind in range(3):
        for there in others:
            in_copy(kind, there).wait_send()
    for stage in range(STEPS + 1):
        both_sides(has_z, lambda side: z_copy(stage, side), "wait_send")
        if stage:
            both_sides(has_x, lambda side: x_copy(stage, side), "wait_send")
    reduce_drain(gram0, 0)
    for j in range(STEPS):
        reduce_drain(gram, j)
    for there in others:
        for kind in range(2):
            out_copy(kind, there).wait_send()


def split_count(n):
    out = []
    while n > 1:
        f = next(f for f in (16, 8, 4, 2, n) if n % f == 0)
        out.append(f)
        n //= f
    return out


def solution(mesh):
    n = mesh.shape["grid"]

    def on_device(right_sides, recycle, medium, shift_table, shift_index):
        block = right_sides.shape[0] // 2
        k_rows = recycle.shape[1]
        lines = right_sides.shape[2]
        cells = lines * right_sides.shape[3]
        quarters = next(q for q in (4, 2, 1) if n % (2 * q) == 0 and lines % q == 0)
        planes = 2 * quarters
        stages, stride = [], 2
        for f in split_count(n // 2):
            stages.append((f, stride))
            stride *= f
        pad = -(-k_rows // block) * block
        ci = cells // quarters
        cw = ci + 2 * LANES
        width = pad + block * (STEPS + 1)
        b = right_sides.reshape(2, block, lines, right_sides.shape[3])
        u = recycle.reshape(2, k_rows, lines, right_sides.shape[3])
        slots = sum(f for f, _ in stages)
        vmem = pl.BlockSpec(memory_space=pltpu.VMEM)
        hbm = pl.BlockSpec(memory_space=pltpu.HBM)
        shape = jax.ShapeDtypeStruct(b.shape, jnp.float32)
        f32, half = jnp.float32, jnp.bfloat16
        sems = lambda *s: pltpu.SemaphoreType.DMA(s)
        sol, res = pl.pallas_call(
            functools.partial(kernel, n, quarters, tuple(stages)),
            out_shape=(shape, shape),
            in_specs=[hbm] * 5,
            out_specs=(vmem, vmem),
            scratch_shapes=[
                pltpu.VMEM(u.shape, f32),
                pltpu.VMEM(b.shape, f32),
                pltpu.VMEM((1, cells), f32),
                pltpu.SMEM(shift_table.shape, f32),
                pltpu.SMEM(shift_index.shape, jnp.int32),
                pltpu.VMEM((2, k_rows, cells + 2 * LANES), f32),
                pltpu.VMEM((2, block, cells), f32),
                pltpu.VMEM((2, block, cells), f32),
                pltpu.VMEM((2, block, cells), f32),
                pltpu.VMEM((planes + 2, k_rows, cw), f32),
                pltpu.VMEM((STEPS, planes + 2, block, cw), f32),
                pltpu.VMEM((planes, block, ci), f32),
                pltpu.VMEM((planes, 1, ci), f32),
                pltpu.VMEM((planes, width, ci), half),
                pltpu.VMEM((planes, width, ci), half),
                pltpu.VMEM((planes, pad, ci), half),
                pltpu.VMEM((planes, pad, ci), half),
                pltpu.VMEM((planes, 2 * block, ci), f32),
                pltpu.VMEM((1, slots, k_rows, LANES), f32),
                pltpu.VMEM((STEPS, slots, block, LANES), f32),
                pltpu.VMEM((block, LANES), f32),
                pltpu.VMEM((block * STEPS, LANES), f32),
                pltpu.VMEM((block * STEPS, pad), f32),
                pltpu.VMEM((block * (STEPS - 1), LANES), f32),
                pltpu.VMEM((pad, LANES), f32),
                pltpu.VMEM((block, pad), f32),
                sems(5),
                sems(3, planes), sems(3, planes),
                sems(STEPS + 1, 2), sems(STEPS + 1, 2),
                sems(STEPS, 2), sems(STEPS, 2),
                sems(STEPS + 1, slots), sems(STEPS + 1, slots),
                sems(2, planes), sems(2, planes),
            ],
            compiler_params=pltpu.CompilerParams(
                collective_id=0, has_side_effects=True, vmem_limit_bytes=65000000
            ),
        )(u, b, medium.reshape(1, cells), shift_table, shift_index)
        return sol.reshape(right_sides.shape), res.reshape(right_sides.shape)

    rows = P(None, "grid", None, None)
    return jax.shard_map(
        on_device,
        mesh=mesh,
        in_specs=(rows, P(None, None, "grid", None, None), P("grid", None, None), P(), P()),
        out_specs=(rows, rows),
        check_vma=False,
    )
```

```python
import functools

import jax
import jax.numpy as jnp
from jax import lax
from jax.experimental import pallas as pl
from jax.experimental.pallas import tpu as pltpu
from jax.sharding import PartitionSpec as P

STEPS = 3
LANES = 128
MESH = pl.DeviceIdType.MESH
highest = lax.Precision.HIGHEST


def dot(left, right):
    return lax.dot_general(
        left, right, (((1,), (0,)), ((), ())), precision=highest, preferred_element_type=jnp.float32
    )


def dot_t(left, right):
    return lax.dot_general(
        left, right, (((1,), (1,)), ((), ())), precision=highest, preferred_element_type=jnp.float32
    )


def halves(x):
    high = x.astype(jnp.bfloat16)
    return high, (x - high.astype(jnp.float32)).astype(jnp.bfloat16)


def thirds(x):
    high, low = halves(x)
    return high, low, (x - high.astype(jnp.float32) - low.astype(jnp.float32)).astype(jnp.bfloat16)


def one(left, right):
    return jnp.dot(left, right, preferred_element_type=jnp.float32)


def one_t(left, right):
    return lax.dot_general(left, right, (((1,), (1,)), ((), ())), preferred_element_type=jnp.float32)


def iota2(shape, dim):
    return lax.broadcasted_iota(jnp.int32, shape, dim)


def eye(size):
    return jnp.where(iota2((size, size), 0) == iota2((size, size), 1), 1.0, 0.0)


def pair_step(x, k, first, second):
    b1 = jnp.broadcast_to(x[:, k : k + 1], x.shape)
    b2 = jnp.broadcast_to(x[:, k + 1 : k + 2], x.shape)
    p12 = b2[k : k + 1]
    i1 = 1.0 / b1[k : k + 1]
    link = b1[k + 1 : k + 2] * i1
    i2 = 1.0 / (b2[k + 1 : k + 2] - link * p12)
    f1 = jnp.where(first, b1 * i1, 0.0)
    f2 = jnp.where(second, (b2 - f1 * p12) * i2, 0.0)
    r1 = x[k : k + 1, :]
    r2 = x[k + 1 : k + 2, :] - link * r1
    return x - f1 * r1 - f2 * r2


def beside(matrix, offset):
    size = matrix.shape[0]
    shape = (size, LANES)
    return jnp.where(iota2(shape, 1) == iota2(shape, 0) + offset, 1.0, matrix)


def factor(x, size, count):
    rows = iota2((size, 1), 0)
    diagonal = iota2((size, LANES), 1) == rows
    for k in range(0, count, 2):
        x = pair_step(x, k, rows > k, rows > k + 1)
    pivots = jnp.sum(jnp.where(diagonal, x, 0.0), axis=1, keepdims=True)
    root = jnp.where(rows < count, lax.rsqrt(jnp.where(rows < count, pivots, 1.0)), 0.0)
    x = x * root
    upper = iota2((size, size), 1) >= iota2((size, size), 0)
    return jnp.where(upper, x[:, 0:size], 0.0), x[:, size : 2 * size]


def eliminate(x, size):
    rows = iota2((size, 1), 0)
    for k in range(0, size, 2):
        x = pair_step(x, k, rows != k, rows != k + 1)
    diagonal = iota2((size, LANES), 1) == rows
    return x / jnp.sum(jnp.where(diagonal, x, 0.0), axis=1, keepdims=True)


def gray(j):
    return j + (j // 2) * (1 - 2 * lax.rem(j, 2))


def flip(t, d, bits):
    out = t
    for b in range(bits):
        out = out + (1 << b) * ((d >> b) & 1) * (1 - 2 * lax.rem(t // (1 << b), 2))
    return out


def kernel(
    n, quarters, stages,
    u_hbm, b_hbm, med_hbm, table_hbm, index_hbm, sol_lines, res_lines,
    u_lines, b_lines, med_ref, table_ref, index_ref,
    u_ref, b_ref, sol_ref, res_ref, ubuf, vbuf, bbuf, mbuf, sh, sl, uh, ul, obuf, gram0, gram, coef, hbt, ebt, lsq, yfirst, fin, back,
    in_sem, in_send, in_recv, z_send, z_recv, x_send, x_recv, red_send, red_recv, out_send, out_recv,
):
    me = lax.axis_index("grid")
    planes = 2 * quarters
    bits = planes.bit_length() - 1
    takes = [
        pltpu.make_async_copy(src, dst, in_sem.at[i])
        for i, (src, dst) in enumerate((
            (u_hbm, u_lines), (b_hbm, b_lines), (med_hbm, med_ref), (table_hbm, table_ref), (index_hbm, index_ref)
        ))
    ]
    for take in takes:
        take.start()
    k_rows = u_ref.shape[1]
    block = b_ref.shape[1]
    cells = b_ref.shape[2]
    ci = cells // quarters
    cw = ci + 2 * LANES
    tiles = ci // LANES
    pad = -(-k_rows // block) * block
    layers = n // planes
    lay, t = me // planes, lax.rem(me, planes)
    base = lay * planes
    core, q = lax.rem(t, 2), gray(t // 2)
    has_z = (lay > 0, lay < layers - 1)
    has_x = (q > 0, q < quarters - 1)
    z_to = (me - planes, me + planes)
    x_to = tuple(base + 2 * gray(q + s) + core for s in (-1, 1))

    barrier = pltpu.get_barrier_semaphore()
    peers = []
    for f, stride in stages:
        mine = lax.rem(me // stride, f)
        peers.append((f, stride, mine, me - mine * stride))
    greet = [base + flip(t, d, bits) for d in range(1, planes)]
    for f, stride, mine, first in peers:
        greet += [first + lax.rem(mine + d, f) * stride for d in range(1, f)]
    if layers > 1:
        greet += [lax.rem(me + planes, n), lax.rem(me + n - planes, n)]
    for to in greet:
        pl.semaphore_signal(barrier, inc=1, device_id=(to,), device_id_type=MESH)

    lines = cells // LANES
    for g in range(2):
        u_ref[g, :, 0:LANES] = jnp.zeros((k_rows, LANES), jnp.float32)
        u_ref[g, :, cells + LANES :] = jnp.zeros((k_rows, LANES), jnp.float32)

    def take_u(x, carry):
        after = pl.ds(pl.multiple_of(x * LANES + LANES, LANES), LANES)
        for g in range(2):
            u_ref[g, :, after] = u_lines[g, :, x, :]
        return carry

    def take_b(x, carry):
        at = pl.ds(pl.multiple_of(x * LANES, LANES), LANES)
        for g in range(2):
            b_ref[g, :, at] = b_lines[g, :, x, :]
        return carry

    takes[0].wait()
    lax.fori_loop(0, lines, take_u, 0, unroll=4)
    for take in takes[1:]:
        take.wait()
    pl.semaphore_wait(barrier, len(greet))

    def part(qq, width):
        return pl.ds(pl.multiple_of(qq * ci, LANES), width)

    def in_copy(kind, there):
        to_core, to_q = lax.rem(there, 2), gray(there // 2)
        if kind == 0:
            src, dst = u_ref.at[to_core, :, part(to_q, cw)], ubuf.at[1 + t]
        elif kind == 1:
            src, dst = med_ref.at[:, part(to_q, ci)], mbuf.at[t]
        else:
            src, dst = b_ref.at[to_core, :, part(to_q, ci)], bbuf.at[t]
        return pltpu.make_async_remote_copy(
            src_ref=src, dst_ref=dst, send_sem=in_send.at[kind, there], recv_sem=in_recv.at[kind, t],
            device_id=(base + there,), device_id_type=MESH,
        )

    def in_wait(kind, there):
        dst = (ubuf.at[1 + there], mbuf.at[there], bbuf.at[there])[kind]
        pltpu.make_async_remote_copy(
            src_ref=dst, dst_ref=dst, send_sem=in_send.at[kind, there], recv_sem=in_recv.at[kind, there],
            device_id=(base + there,), device_id_type=MESH,
        ).wait_recv()

    others = [flip(t, d, bits) for d in range(planes - 1, 0, -1)]
    for kind in range(2):
        for there in others:
            in_copy(kind, there).start()

    lax.fori_loop(0, lines, take_b, 0, unroll=4)
    for there in others:
        in_copy(2, there).start()
    ubuf[1 + t, :, :] = u_ref[core, :, part(q, cw)]
    mbuf[t, :, :] = med_ref[:, part(q, ci)]
    bbuf[t, :, :] = b_ref[core, :, part(q, ci)]

    shift = jnp.float32(0.0)
    for s in range(table_ref.shape[0]):
        shift = shift + jnp.where(index_ref[core] == s, table_ref[s], 0.0)
    shift = 6.0 + shift

    inner = pl.ds(LANES, ci)
    zero_plane = (0, planes + 1)
    for side in range(2):
        @pl.when(jnp.logical_not(has_z[side]))
        def _():
            ubuf[zero_plane[side]] = jnp.zeros(ubuf.shape[1:], jnp.float32)
            for j in range(STEPS):
                vbuf[j, zero_plane[side]] = jnp.zeros(vbuf.shape[2:], jnp.float32)

        @pl.when(jnp.logical_not(has_x[side]))
        def _():
            lanes = pl.ds((0, cw - LANES)[side], LANES)
            for j in range(STEPS):
                vbuf[j, :, :, lanes] = jnp.zeros((planes + 2, block, LANES), jnp.float32)

    def z_copy(stage, side):
        buf = ubuf if stage == 0 else vbuf.at[stage - 1]
        return pltpu.make_async_remote_copy(
            src_ref=buf.at[(1, planes)[side], :, inner], dst_ref=buf.at[(planes + 1, 0)[side], :, inner],
            send_sem=z_send.at[stage, side], recv_sem=z_recv.at[stage, side],
            device_id=(z_to[side],), device_id_type=MESH,
        )

    def x_copy(stage, side):
        buf = vbuf.at[stage - 1]
        mid = pl.ds(1, planes)
        return pltpu.make_async_remote_copy(
            src_ref=buf.at[mid, :, pl.ds((LANES, ci)[side], LANES)],
            dst_ref=buf.at[mid, :, pl.ds((cw - LANES, 0)[side], LANES)],
            send_sem=x_send.at[stage - 1, side], recv_sem=x_recv.at[stage - 1, side],
            device_id=(x_to[side],), device_id_type=MESH,
        )

    def both_sides(has, make, act):
        for side in range(2):
            @pl.when(has[side])
            def _():
                getattr(make(side), act)()

    def halo_start(has, make):
        both_sides(has, make, "start")

    def halo_wait(has, make):
        both_sides(has[::-1], make, "wait_recv")

    def reduce_sum(buffer, number, value, meanwhile=None):
        sem = number if buffer is gram0 else number + 1
        offset = 0
        for f, stride, mine, first in peers:
            own = offset + mine
            buffer[number, own, :, :] = value
            for d in range(1, f):
                to = lax.rem(mine + d, f)
                pltpu.make_async_remote_copy(
                    src_ref=buffer.at[number, own], dst_ref=buffer.at[number, own],
                    send_sem=red_send.at[sem, offset + d], recv_sem=red_recv.at[sem, own],
                    device_id=(first + to * stride,), device_id_type=MESH,
                ).start()
            if meanwhile is not None:
                meanwhile()
                meanwhile = None
            for d in range(1, f):
                there = lax.rem(mine + d, f)
                origin = offset + there
                pltpu.make_async_remote_copy(
                    src_ref=buffer.at[number, origin], dst_ref=buffer.at[number, origin],
                    send_sem=red_send.at[sem, offset + d], recv_sem=red_recv.at[sem, origin],
                    device_id=(first + there * stride,), device_id_type=MESH,
                ).wait_recv()
            value = buffer[number, offset, :, :]
            for s in range(1, f):
                value = value + buffer[number, offset + s, :, :]
            offset += f
        return value

    def reduce_drain(buffer, number):
        sem = number if buffer is gram0 else number + 1
        offset = 0
        for f, stride, mine, first in peers:
            for d in range(1, f):
                pltpu.make_async_remote_copy(
                    src_ref=buffer.at[number, offset + mine], dst_ref=buffer.at[number, offset + mine],
                    send_sem=red_send.at[sem, offset + d], recv_sem=red_recv.at[sem, offset + mine],
                    device_id=(first + lax.rem(mine + d, f) * stride,), device_id_type=MESH,
                ).wait_send()
            offset += f

    lane = iota2((1, LANES), 1)

    def stencil(buf, p, tile):
        load = lambda z, s: buf[z, :, s * LANES : (s + 1) * LANES]
        c = load(p + 1, tile + 1)
        near = load(p + 1, tile) + load(p + 1, tile + 2)
        near = near + load(p, tile + 1) + load(p + 2, tile + 1)
        near = near + jnp.where(lane == 0, 0.0, pltpu.roll(c, 1, 1))
        near = near + jnp.where(lane == LANES - 1, 0.0, pltpu.roll(c, LANES - 1, 1))
        diag = mbuf[p, :, tile * LANES : (tile + 1) * LANES] + shift
        return diag * c - near, c

    def put(high, low, p, row, tile, value):
        at = slice(tile * LANES, (tile + 1) * LANES)
        h, l = halves(value)
        high[p, row : row + value.shape[0], at] = h
        low[p, row : row + value.shape[0], at] = l

    for kind in range(2):
        for there in others:
            in_wait(kind, there)
    halo_start(has_z, lambda side: z_copy(0, side))

    fill = jnp.zeros((pad - k_rows, LANES), jnp.float32)

    def widen(x):
        return jnp.concatenate([x, fill], axis=0) if pad > k_rows else x

    def image_plane(p, carry):
        for tile in range(tiles):
            applied, c = stencil(ubuf, p, tile)
            put(sh, sl, p, 0, tile, widen(applied))
            put(uh, ul, p, 0, tile, widen(c))
        return carry

    if planes > 2:
        lax.fori_loop(1, planes - 1, image_plane, 0)
    halo_wait(has_z, lambda side: z_copy(0, side))
    image_plane(0, 0)
    image_plane(planes - 1, 0)

    for there in others:
        in_wait(2, there)
    size = pad + block

    def first_gram(p, acc):
        for tile in range(tiles):
            put(sh, sl, p, pad, tile, bbuf[p, :, tile * LANES : (tile + 1) * LANES])
        rows = sh[p, 0:size, :]
        return acc + one_t(jnp.concatenate([rows, sl[p, 0:size, :]], axis=0), rows)

    acc = lax.fori_loop(0, planes, first_gram, jnp.zeros((2 * size, size), jnp.float32), unroll=min(4, planes))
    cross = acc[size:, :]
    whole = acc[:size, :] + cross + dot_t(eye(size), cross)
    fin[0:k_rows, 0:size] = whole[0:k_rows, :]
    fin[0:k_rows, size:] = jnp.zeros((k_rows, LANES - size), jnp.float32)
    half = LANES // 2
    fin[0:block, half : half + block] = whole[pad:, pad:]

    def clear():
        hbt[...] = jnp.zeros(hbt.shape, jnp.float32)
        lsq[...] = jnp.zeros(lsq.shape, jnp.float32)

    fin[0:k_rows, :] = reduce_sum(gram0, 0, fin[0:k_rows, :], clear)
    if pad > k_rows:
        fin[k_rows:pad, :] = jnp.zeros((pad - k_rows, LANES), jnp.float32)
    lanes = iota2((pad, LANES), 1)
    mixed = fin[0:pad, 0:size]
    linv = factor(beside(jnp.where(lanes < pad, fin[0:pad, :], 0.0), pad), pad, k_rows)[1]
    whole_inv = lax.dot_general(
        linv, linv, (((0,), (0,)), ((), ())), precision=highest, preferred_element_type=jnp.float32
    )
    ba = dot_t(eye(block), mixed[:, pad:size])
    ba_inv = dot(ba, whole_inv)
    remaining = fin[0:block, half : half + block] - dot_t(ba_inv, ba)
    wide_zero = jnp.zeros((block, LANES - block), jnp.float32)
    full = lambda m: jnp.concatenate([m, wide_zero], axis=1)
    top_factor, inv = factor(beside(full(remaining), block), block, block)
    coef[:, 0:pad] = -dot(inv, ba_inv)
    coef[:, pad:size] = inv

    unit = eye(block)
    lower = dot_t(unit, top_factor)
    for j in range(1, STEPS + 1):
        known = pad + block * j
        stacked = jnp.concatenate(thirds(coef[:, 0:known]), axis=0)

        def combine(p, first_tile, last_tile):
            at = slice(first_tile * LANES, last_tile * LANES)
            first = one(stacked, sh[p, 0:known, at])
            second = one(stacked[0 : 2 * block], sl[p, 0:known, at])
            value = first[0:block] + (first[block : 2 * block] + second[0:block])
            value = value + (first[2 * block :] + second[block:])
            vbuf[j - 1, p + 1, :, LANES + first_tile * LANES : LANES + last_tile * LANES] = value
            for tile in range(first_tile, last_tile):
                here = slice((tile - first_tile) * LANES, (tile - first_tile + 1) * LANES)
                put(sh, sl, p, known - block, tile, value[:, here])

        def combine_edges(p, carry):
            combine(p, 0, 1)
            combine(p, tiles - 1, tiles)
            return carry

        def combine_inner(p, carry):
            combine(p, 1, tiles - 1)
            return carry

        def image_inner(p, carry):
            for tile in range(1, tiles - 1):
                put(sh, sl, p, known, tile, stencil(vbuf.at[j - 1], p, tile)[0])
            return carry

        wide = known + block
        ends = (0, planes - 1)
        acc = jnp.zeros((2 * wide, 2 * block), jnp.float32)

        def gram_of(rows, rest):
            new = jnp.concatenate([rows[known:], rest[known:]], axis=0)
            return one_t(jnp.concatenate([rows, rest], axis=0), new)

        def image(p, tile):
            put(sh, sl, p, known, tile, stencil(vbuf.at[j - 1], p, tile)[0])

        def inner_gram(p, acc):
            for tile in range(1, tiles - 1):
                image(p, tile)
            at = slice(LANES, (tiles - 1) * LANES)
            return acc + gram_of(sh[p, 0:wide, at], sl[p, 0:wide, at])

        for p in ends:
            combine(p, 0, tiles)
        halo_start(has_z, lambda side: z_copy(j, side))
        for p in range(1, planes - 1):
            combine(p, 0, 1)
            combine(p, tiles - 1, tiles)
        halo_start(has_x, lambda side: x_copy(j, side))
        for p in range(1, planes - 1):
            combine(p, 1, tiles - 1)
        if planes > 2:
            acc = lax.fori_loop(1, planes - 1, inner_gram, acc, unroll=(planes - 2) // 2)
        halo_wait(has_x, lambda side: x_copy(j, side))
        lanes_of = lambda ref, p, tile: ref[p, 0:wide, tile * LANES : (tile + 1) * LANES]
        sides = [(p, tile) for p in range(1, planes - 1) for tile in (0, tiles - 1)]
        for p, tile in sides:
            image(p, tile)
        if sides:
            acc = acc + gram_of(*(
                jnp.concatenate([lanes_of(ref, p, tile) for p, tile in sides], axis=1) for ref in (sh, sl)
            ))
        halo_wait(has_z, lambda side: z_copy(j, side))
        for p in ends:
            for tile in range(tiles):
                image(p, tile)
            acc = acc + gram_of(sh[p, 0:wide, :], sl[p, 0:wide, :])
        tall = acc[0:wide, 0:block] + (acc[wide:, 0:block] + acc[0:wide, block:] + acc[wide:, block:])
        fin[0:block, 0:wide] = dot_t(unit, tall)
        early = block * (STEPS - 1)

        if j == STEPS:
            pads = jnp.zeros((early, LANES - early), jnp.float32)

            def invert_early():
                he = hbt[0:early, :]
                normal = jnp.concatenate([dot_t(he, he), pads], axis=1)
                lsq[...] = eliminate(beside(normal, early), early)
                yfirst[...] = dot(dot_t(lower, he[:, 0:block]), lsq[:, early : 2 * early])

            fin[0:block, :] = reduce_sum(gram, j - 1, fin[0:block, :], invert_early)
        else:
            fin[0:block, :] = reduce_sum(gram, j - 1, fin[0:block, :])
        wa = fin[0:block, 0:pad]
        wa_inv = dot(wa, whole_inv)
        ht = fin[0:block, pad:known]
        at = block * (j - 1)
        ebt[at : at + block, :] = wa_inv
        outside = fin[0:block, known:wide] - dot_t(wa_inv, wa)
        if j == STEPS:
            break
        fresh = outside - dot_t(ht, ht)
        lt, inv = factor(beside(full(fresh), block), block, block)
        coef[:, 0:pad] = -dot(inv, wa_inv)
        coef[:, pad:known] = -dot(inv, ht)
        coef[:, known:wide] = inv
        hbt[at : at + block, 0 : known - pad] = ht
        hbt[at : at + block, known - pad : known - pad + block] = dot_t(unit, lt)

    width = pad + block * (STEPS + 1)
    kry = block * STEPS
    he, yt0 = hbt[0:early, 0:kry], yfirst[...]
    p = lsq[:, early : 2 * early]
    cross = dot_t(ht, he)
    bent = dot(cross, p)
    schur = outside - dot_t(bent, cross)
    late_right = dot_t(lower, ht[:, 0:block]) - dot_t(yt0, cross)
    both = jnp.concatenate([schur, dot_t(unit, late_right), wide_zero[:, block:]], axis=1)
    y_late = dot_t(unit, eliminate(both, block)[:, block : 2 * block])
    y_early = yt0 - dot(y_late, bent)
    yt = jnp.concatenate([y_early, y_late], axis=1)
    back[...] = ba_inv - dot(yt, ebt[...])
    fin[...] = jnp.zeros(fin.shape, jnp.float32)
    fin[0:block, pad : pad + kry] = yt
    fin[block : 2 * block, 0:pad] = dot(y_late, wa_inv)
    fin[block : 2 * block, pad : pad + kry] = -dot(y_early, he)
    fin[block : 2 * block, pad : pad + block] = fin[block : 2 * block, pad : pad + block] + lower
    fin[block : 2 * block, pad + kry : width] = -y_late
    high, low = halves(fin[0 : 2 * block, 0:width])
    stacked = jnp.concatenate([high, low], axis=0)
    bh, bl = halves(back[...])
    bstack = jnp.concatenate([bh, bl], axis=0)

    def out_copy(kind, there):
        dst = (sol_ref, res_ref)[kind]
        return pltpu.make_async_remote_copy(
            src_ref=obuf.at[there, pl.ds(kind * block, block)], dst_ref=dst.at[core, :, part(q, ci)],
            send_sem=out_send.at[kind, there], recv_sem=out_recv.at[kind, t],
            device_id=(base + there,), device_id_type=MESH,
        )

    def out_wait(kind, there):
        dst = (sol_ref, res_ref)[kind].at[lax.rem(there, 2), :, part(gray(there // 2), ci)]
        pltpu.make_async_remote_copy(
            src_ref=dst, dst_ref=dst, send_sem=out_send.at[kind, there], recv_sem=out_recv.at[kind, there],
            device_id=(base + there,), device_id_type=MESH,
        ).wait_recv()

    def final_plane(p):
        first = one(stacked, sh[p, 0:width, :])
        both = first[0 : 2 * block] + (first[2 * block :] + one(high, sl[p, 0:width, :]))
        first = one(bstack, uh[p])
        return both[0:block] + (first[0:block] + (first[block:] + one(bh, ul[p]))), both[block:]

    def final_send(i, carry):
        there = flip(t, planes - 1 - i, bits)
        sol, res = final_plane(there)
        obuf[there, 0:block, :] = sol
        obuf[there, block:, :] = res
        for kind in range(2):
            out_copy(kind, there).start()
        return carry

    lax.fori_loop(0, planes - 1, final_send, 0)
    sol, res = final_plane(t)
    for x in range(tiles):
        sol_lines[core, :, q * tiles + x, :] = sol[:, x * LANES : (x + 1) * LANES]
        res_lines[core, :, q * tiles + x, :] = res[:, x * LANES : (x + 1) * LANES]

    for there in others:
        g, first_line = lax.rem(there, 2), gray(there // 2) * tiles
        for kind in range(2):
            out_wait(kind, there)
            landed, lines_of = (sol_ref, sol_lines, res_ref, res_lines)[2 * kind : 2 * kind + 2]
            for x in range(tiles):
                at = pl.ds(pl.multiple_of((first_line + x) * LANES, LANES), LANES)
                lines_of[g, :, first_line + x, :] = landed[g, :, at]
    for kind in range(3):
        for there in others:
            in_copy(kind, there).wait_send()
    for stage in range(STEPS + 1):
        both_sides(has_z, lambda side: z_copy(stage, side), "wait_send")
        if stage:
            both_sides(has_x, lambda side: x_copy(stage, side), "wait_send")
    reduce_drain(gram0, 0)
    for j in range(STEPS):
        reduce_drain(gram, j)
    for there in others:
        for kind in range(2):
            out_copy(kind, there).wait_send()


def split_count(n):
    out = []
    while n > 1:
        f = next(f for f in (16, 8, 4, 2, n) if n % f == 0)
        out.append(f)
        n //= f
    return out


def solution(mesh):
    n = mesh.shape["grid"]

    def on_device(right_sides, recycle, medium, shift_table, shift_index):
        block = right_sides.shape[0] // 2
        k_rows = recycle.shape[1]
        lines = right_sides.shape[2]
        cells = lines * right_sides.shape[3]
        quarters = next(q for q in (4, 2, 1) if n % (2 * q) == 0 and lines % q == 0)
        planes = 2 * quarters
        stages, stride = [], 2
        for f in split_count(n // 2):
            stages.append((f, stride))
            stride *= f
        pad = -(-k_rows // block) * block
        ci = cells // quarters
        cw = ci + 2 * LANES
        width = pad + block * (STEPS + 1)
        b = right_sides.reshape(2, block, lines, right_sides.shape[3])
        u = recycle.reshape(2, k_rows, lines, right_sides.shape[3])
        slots = sum(f for f, _ in stages)
        vmem = pl.BlockSpec(memory_space=pltpu.VMEM)
        hbm = pl.BlockSpec(memory_space=pltpu.HBM)
        shape = jax.ShapeDtypeStruct(b.shape, jnp.float32)
        f32, half = jnp.float32, jnp.bfloat16
        sems = lambda *s: pltpu.SemaphoreType.DMA(s)
        sol, res = pl.pallas_call(
            functools.partial(kernel, n, quarters, tuple(stages)),
            out_shape=(shape, shape),
            in_specs=[hbm] * 5,
            out_specs=(vmem, vmem),
            scratch_shapes=[
                pltpu.VMEM(u.shape, f32),
                pltpu.VMEM(b.shape, f32),
                pltpu.VMEM((1, cells), f32),
                pltpu.SMEM(shift_table.shape, f32),
                pltpu.SMEM(shift_index.shape, jnp.int32),
                pltpu.VMEM((2, k_rows, cells + 2 * LANES), f32),
                pltpu.VMEM((2, block, cells), f32),
                pltpu.VMEM((2, block, cells), f32),
                pltpu.VMEM((2, block, cells), f32),
                pltpu.VMEM((planes + 2, k_rows, cw), f32),
                pltpu.VMEM((STEPS, planes + 2, block, cw), f32),
                pltpu.VMEM((planes, block, ci), f32),
                pltpu.VMEM((planes, 1, ci), f32),
                pltpu.VMEM((planes, width, ci), half),
                pltpu.VMEM((planes, width, ci), half),
                pltpu.VMEM((planes, pad, ci), half),
                pltpu.VMEM((planes, pad, ci), half),
                pltpu.VMEM((planes, 2 * block, ci), f32),
                pltpu.VMEM((1, slots, k_rows, LANES), f32),
                pltpu.VMEM((STEPS, slots, block, LANES), f32),
                pltpu.VMEM((block, LANES), f32),
                pltpu.VMEM((block * STEPS, LANES), f32),
                pltpu.VMEM((block * STEPS, pad), f32),
                pltpu.VMEM((block * (STEPS - 1), LANES), f32),
                pltpu.VMEM((block, block * (STEPS - 1)), f32),
                pltpu.VMEM((pad, LANES), f32),
                pltpu.VMEM((block, pad), f32),
                sems(5),
                sems(3, planes), sems(3, planes),
                sems(STEPS + 1, 2), sems(STEPS + 1, 2),
                sems(STEPS, 2), sems(STEPS, 2),
                sems(STEPS + 1, slots), sems(STEPS + 1, slots),
                sems(2, planes), sems(2, planes),
            ],
            compiler_params=pltpu.CompilerParams(
                collective_id=0, has_side_effects=True, vmem_limit_bytes=65000000
            ),
        )(u, b, medium.reshape(1, cells), shift_table, shift_index)
        return sol.reshape(right_sides.shape), res.reshape(right_sides.shape)

    rows = P(None, "grid", None, None)
    return jax.shard_map(
        on_device,
        mesh=mesh,
        in_specs=(rows, P(None, None, "grid", None, None), P("grid", None, None), P(), P()),
        out_specs=(rows, rows),
        check_vma=False,
    )
```

```python
import functools

import jax
import jax.numpy as jnp
from jax import lax
from jax.experimental import pallas as pl
from jax.experimental.pallas import tpu as pltpu
from jax.sharding import PartitionSpec as P

STEPS = 3
LANES = 128
MESH = pl.DeviceIdType.MESH
highest = lax.Precision.HIGHEST


def dot(left, right):
    return lax.dot_general(
        left, right, (((1,), (0,)), ((), ())), precision=highest, preferred_element_type=jnp.float32
    )


def dot_t(left, right):
    return lax.dot_general(
        left, right, (((1,), (1,)), ((), ())), precision=highest, preferred_element_type=jnp.float32
    )


def halves(x):
    high = x.astype(jnp.bfloat16)
    return high, (x - high.astype(jnp.float32)).astype(jnp.bfloat16)


def thirds(x):
    high, low = halves(x)
    return high, low, (x - high.astype(jnp.float32) - low.astype(jnp.float32)).astype(jnp.bfloat16)


def one(left, right):
    return jnp.dot(left, right, preferred_element_type=jnp.float32)


def one_t(left, right):
    return lax.dot_general(left, right, (((1,), (1,)), ((), ())), preferred_element_type=jnp.float32)


def iota2(shape, dim):
    return lax.broadcasted_iota(jnp.int32, shape, dim)


def eye(size):
    return jnp.where(iota2((size, size), 0) == iota2((size, size), 1), 1.0, 0.0)


def pair_step(x, k, first, second):
    b1 = jnp.broadcast_to(x[:, k : k + 1], x.shape)
    b2 = jnp.broadcast_to(x[:, k + 1 : k + 2], x.shape)
    p12 = b2[k : k + 1]
    i1 = 1.0 / b1[k : k + 1]
    link = b1[k + 1 : k + 2] * i1
    i2 = 1.0 / (b2[k + 1 : k + 2] - link * p12)
    f1 = jnp.where(first, b1 * i1, 0.0)
    f2 = jnp.where(second, (b2 - f1 * p12) * i2, 0.0)
    r1 = x[k : k + 1, :]
    r2 = x[k + 1 : k + 2, :] - link * r1
    return x - f1 * r1 - f2 * r2


def beside(matrix, offset):
    size = matrix.shape[0]
    shape = (size, LANES)
    return jnp.where(iota2(shape, 1) == iota2(shape, 0) + offset, 1.0, matrix)


def factor(x, size, count):
    rows = iota2((size, 1), 0)
    diagonal = iota2((size, LANES), 1) == rows
    for k in range(0, count, 2):
        x = pair_step(x, k, rows > k, rows > k + 1)
    pivots = jnp.sum(jnp.where(diagonal, x, 0.0), axis=1, keepdims=True)
    root = jnp.where(rows < count, lax.rsqrt(jnp.where(rows < count, pivots, 1.0)), 0.0)
    x = x * root
    upper = iota2((size, size), 1) >= iota2((size, size), 0)
    return jnp.where(upper, x[:, 0:size], 0.0), x[:, size : 2 * size]


def eliminate(x, size):
    rows = iota2((size, 1), 0)
    for k in range(0, size, 2):
        x = pair_step(x, k, rows != k, rows != k + 1)
    diagonal = iota2((size, LANES), 1) == rows
    return x / jnp.sum(jnp.where(diagonal, x, 0.0), axis=1, keepdims=True)


def gray(j):
    return j + (j // 2) * (1 - 2 * lax.rem(j, 2))


def flip(t, d, bits):
    out = t
    for b in range(bits):
        out = out + (1 << b) * ((d >> b) & 1) * (1 - 2 * lax.rem(t // (1 << b), 2))
    return out


def kernel(
    n, quarters, stages,
    u_hbm, b_hbm, med_hbm, table_hbm, index_hbm, sol_lines, res_lines,
    u_lines, b_lines, med_ref, table_ref, index_ref,
    u_ref, b_ref, sol_ref, res_ref, ubuf, vbuf, bbuf, mbuf, sh, sl, uh, ul, obuf, gram0, gram, coef, hbt, ebt, lsq, yfirst, aug, fin, back,
    in_sem, in_send, in_recv, z_send, z_recv, x_send, x_recv, red_send, red_recv, out_send, out_recv,
):
    me = lax.axis_index("grid")
    planes = 2 * quarters
    bits = planes.bit_length() - 1
    takes = [
        pltpu.make_async_copy(src, dst, in_sem.at[i])
        for i, (src, dst) in enumerate((
            (u_hbm, u_lines), (b_hbm, b_lines), (med_hbm, med_ref), (table_hbm, table_ref), (index_hbm, index_ref)
        ))
    ]
    for take in takes:
        take.start()
    k_rows = u_ref.shape[1]
    block = b_ref.shape[1]
    cells = b_ref.shape[2]
    ci = cells // quarters
    cw = ci + 2 * LANES
    tiles = ci // LANES
    pad = -(-k_rows // block) * block
    layers = n // planes
    lay, t = me // planes, lax.rem(me, planes)
    base = lay * planes
    core, q = lax.rem(t, 2), gray(t // 2)
    has_z = (lay > 0, lay < layers - 1)
    has_x = (q > 0, q < quarters - 1)
    z_to = (me - planes, me + planes)
    x_to = tuple(base + 2 * gray(q + s) + core for s in (-1, 1))

    barrier = pltpu.get_barrier_semaphore()
    peers = []
    for f, stride in stages:
        mine = lax.rem(me // stride, f)
        peers.append((f, stride, mine, me - mine * stride))
    greet = [base + flip(t, d, bits) for d in range(1, planes)]
    for f, stride, mine, first in peers:
        greet += [first + lax.rem(mine + d, f) * stride for d in range(1, f)]
    if layers > 1:
        greet += [lax.rem(me + planes, n), lax.rem(me + n - planes, n)]
    for to in greet:
        pl.semaphore_signal(barrier, inc=1, device_id=(to,), device_id_type=MESH)

    lines = cells // LANES
    for g in range(2):
        u_ref[g, :, 0:LANES] = jnp.zeros((k_rows, LANES), jnp.float32)
        u_ref[g, :, cells + LANES :] = jnp.zeros((k_rows, LANES), jnp.float32)

    def take_u(x, carry):
        after = pl.ds(pl.multiple_of(x * LANES + LANES, LANES), LANES)
        for g in range(2):
            u_ref[g, :, after] = u_lines[g, :, x, :]
        return carry

    def take_b(x, carry):
        at = pl.ds(pl.multiple_of(x * LANES, LANES), LANES)
        for g in range(2):
            b_ref[g, :, at] = b_lines[g, :, x, :]
        return carry

    takes[0].wait()
    lax.fori_loop(0, lines, take_u, 0, unroll=4)
    for take in takes[1:]:
        take.wait()
    pl.semaphore_wait(barrier, len(greet))

    def part(qq, width):
        return pl.ds(pl.multiple_of(qq * ci, LANES), width)

    def in_copy(kind, there):
        to_core, to_q = lax.rem(there, 2), gray(there // 2)
        if kind == 0:
            src, dst = u_ref.at[to_core, :, part(to_q, cw)], ubuf.at[1 + t]
        elif kind == 1:
            src, dst = med_ref.at[:, part(to_q, ci)], mbuf.at[t]
        else:
            src, dst = b_ref.at[to_core, :, part(to_q, ci)], bbuf.at[t]
        return pltpu.make_async_remote_copy(
            src_ref=src, dst_ref=dst, send_sem=in_send.at[kind, there], recv_sem=in_recv.at[kind, t],
            device_id=(base + there,), device_id_type=MESH,
        )

    def in_wait(kind, there):
        dst = (ubuf.at[1 + there], mbuf.at[there], bbuf.at[there])[kind]
        pltpu.make_async_remote_copy(
            src_ref=dst, dst_ref=dst, send_sem=in_send.at[kind, there], recv_sem=in_recv.at[kind, there],
            device_id=(base + there,), device_id_type=MESH,
        ).wait_recv()

    others = [flip(t, d, bits) for d in range(planes - 1, 0, -1)]
    for kind in range(2):
        for there in others:
            in_copy(kind, there).start()

    lax.fori_loop(0, lines, take_b, 0, unroll=4)
    for there in others:
        in_copy(2, there).start()
    ubuf[1 + t, :, :] = u_ref[core, :, part(q, cw)]
    mbuf[t, :, :] = med_ref[:, part(q, ci)]
    bbuf[t, :, :] = b_ref[core, :, part(q, ci)]

    shift = jnp.float32(0.0)
    for s in range(table_ref.shape[0]):
        shift = shift + jnp.where(index_ref[core] == s, table_ref[s], 0.0)
    shift = 6.0 + shift

    inner = pl.ds(LANES, ci)
    zero_plane = (0, planes + 1)
    for side in range(2):
        @pl.when(jnp.logical_not(has_z[side]))
        def _():
            ubuf[zero_plane[side]] = jnp.zeros(ubuf.shape[1:], jnp.float32)
            for j in range(STEPS):
                vbuf[j, zero_plane[side]] = jnp.zeros(vbuf.shape[2:], jnp.float32)

        @pl.when(jnp.logical_not(has_x[side]))
        def _():
            lanes = pl.ds((0, cw - LANES)[side], LANES)
            for j in range(STEPS):
                vbuf[j, :, :, lanes] = jnp.zeros((planes + 2, block, LANES), jnp.float32)

    def z_copy(stage, side):
        buf = ubuf if stage == 0 else vbuf.at[stage - 1]
        return pltpu.make_async_remote_copy(
            src_ref=buf.at[(1, planes)[side], :, inner], dst_ref=buf.at[(planes + 1, 0)[side], :, inner],
            send_sem=z_send.at[stage, side], recv_sem=z_recv.at[stage, side],
            device_id=(z_to[side],), device_id_type=MESH,
        )

    def x_copy(stage, side):
        buf = vbuf.at[stage - 1]
        mid = pl.ds(1, planes)
        return pltpu.make_async_remote_copy(
            src_ref=buf.at[mid, :, pl.ds((LANES, ci)[side], LANES)],
            dst_ref=buf.at[mid, :, pl.ds((cw - LANES, 0)[side], LANES)],
            send_sem=x_send.at[stage - 1, side], recv_sem=x_recv.at[stage - 1, side],
            device_id=(x_to[side],), device_id_type=MESH,
        )

    def both_sides(has, make, act):
        for side in range(2):
            @pl.when(has[side])
            def _():
                getattr(make(side), act)()

    def halo_start(has, make):
        both_sides(has, make, "start")

    def halo_wait(has, make):
        both_sides(has[::-1], make, "wait_recv")

    def reduce_sum(buffer, number, value, meanwhile=None):
        sem = number if buffer is gram0 else number + 1
        offset = 0
        for f, stride, mine, first in peers:
            own = offset + mine
            buffer[number, own, :, :] = value
            for d in range(1, f):
                to = lax.rem(mine + d, f)
                pltpu.make_async_remote_copy(
                    src_ref=buffer.at[number, own], dst_ref=buffer.at[number, own],
                    send_sem=red_send.at[sem, offset + d], recv_sem=red_recv.at[sem, own],
                    device_id=(first + to * stride,), device_id_type=MESH,
                ).start()
            if meanwhile is not None:
                meanwhile()
                meanwhile = None
            for d in range(1, f):
                there = lax.rem(mine + d, f)
                origin = offset + there
                pltpu.make_async_remote_copy(
                    src_ref=buffer.at[number, origin], dst_ref=buffer.at[number, origin],
                    send_sem=red_send.at[sem, offset + d], recv_sem=red_recv.at[sem, origin],
                    device_id=(first + there * stride,), device_id_type=MESH,
                ).wait_recv()
            value = buffer[number, offset, :, :]
            for s in range(1, f):
                value = value + buffer[number, offset + s, :, :]
            offset += f
        return value

    def reduce_drain(buffer, number):
        sem = number if buffer is gram0 else number + 1
        offset = 0
        for f, stride, mine, first in peers:
            for d in range(1, f):
                pltpu.make_async_remote_copy(
                    src_ref=buffer.at[number, offset + mine], dst_ref=buffer.at[number, offset + mine],
                    send_sem=red_send.at[sem, offset + d], recv_sem=red_recv.at[sem, offset + mine],
                    device_id=(first + lax.rem(mine + d, f) * stride,), device_id_type=MESH,
                ).wait_send()
            offset += f

    lane = iota2((1, LANES), 1)

    def stencil(buf, p, tile):
        load = lambda z, s: buf[z, :, s * LANES : (s + 1) * LANES]
        c = load(p + 1, tile + 1)
        near = load(p + 1, tile) + load(p + 1, tile + 2)
        near = near + load(p, tile + 1) + load(p + 2, tile + 1)
        near = near + jnp.where(lane == 0, 0.0, pltpu.roll(c, 1, 1))
        near = near + jnp.where(lane == LANES - 1, 0.0, pltpu.roll(c, LANES - 1, 1))
        diag = mbuf[p, :, tile * LANES : (tile + 1) * LANES] + shift
        return diag * c - near, c

    def put(high, low, p, row, tile, value):
        at = slice(tile * LANES, (tile + 1) * LANES)
        h, l = halves(value)
        high[p, row : row + value.shape[0], at] = h
        low[p, row : row + value.shape[0], at] = l

    for kind in range(2):
        for there in others:
            in_wait(kind, there)
    halo_start(has_z, lambda side: z_copy(0, side))

    fill = jnp.zeros((pad - k_rows, LANES), jnp.float32)

    def widen(x):
        return jnp.concatenate([x, fill], axis=0) if pad > k_rows else x

    def image_plane(p, carry):
        for tile in range(tiles):
            applied, c = stencil(ubuf, p, tile)
            put(sh, sl, p, 0, tile, widen(applied))
            put(uh, ul, p, 0, tile, widen(c))
        return carry

    if planes > 2:
        lax.fori_loop(1, planes - 1, image_plane, 0)
    halo_wait(has_z, lambda side: z_copy(0, side))
    image_plane(0, 0)
    image_plane(planes - 1, 0)

    for there in others:
        in_wait(2, there)
    size = pad + block

    def first_gram(p, acc):
        for tile in range(tiles):
            put(sh, sl, p, pad, tile, bbuf[p, :, tile * LANES : (tile + 1) * LANES])
        rows = sh[p, 0:size, :]
        return acc + one_t(jnp.concatenate([rows, sl[p, 0:size, :]], axis=0), rows)

    acc = lax.fori_loop(0, planes, first_gram, jnp.zeros((2 * size, size), jnp.float32), unroll=min(4, planes))
    cross = acc[size:, :]
    whole = acc[:size, :] + cross + dot_t(eye(size), cross)
    fin[0:k_rows, 0:size] = whole[0:k_rows, :]
    fin[0:k_rows, size:] = jnp.zeros((k_rows, LANES - size), jnp.float32)
    half = LANES // 2
    fin[0:block, half : half + block] = whole[pad:, pad:]
    after = half + block
    fin[0:block, after : after + pad] = whole[pad:, 0:pad]

    def clear():
        hbt[...] = jnp.zeros(hbt.shape, jnp.float32)
        lsq[...] = jnp.zeros(lsq.shape, jnp.float32)

    fin[0:k_rows, :] = reduce_sum(gram0, 0, fin[0:k_rows, :], clear)
    rows, at_lane = iota2((size, LANES), 0), iota2((size, LANES), 1)
    aug[...] = jnp.where((at_lane == rows + size) & (rows < k_rows), 1.0, 0.0)
    aug[0:k_rows, 0:size] = fin[0:k_rows, 0:size]
    aug[pad:size, 0:pad] = fin[0:block, after : after + pad]
    aug[pad:size, pad:size] = fin[0:block, half : half + block]
    x, row = aug[...], rows[:, 0:1]
    for k in range(0, k_rows, 2):
        x = pair_step(x, k, row != k, row != k + 1)
    pivots = jnp.sum(jnp.where(at_lane == rows, x, 0.0), axis=1, keepdims=True)
    scale = jnp.where(row < k_rows, 1.0 / jnp.where(row < k_rows, pivots, 1.0), 0.0)
    whole_inv = (x * scale)[0:pad, size : size + pad]
    ba_inv = -x[pad:size, size : size + pad]
    remaining = x[pad:size, pad:size]
    wide_zero = jnp.zeros((block, LANES - block), jnp.float32)
    full = lambda m: jnp.concatenate([m, wide_zero], axis=1)
    top_factor, inv = factor(beside(full(remaining), block), block, block)
    coef[:, 0:pad] = -dot(inv, ba_inv)
    coef[:, pad:size] = inv

    unit = eye(block)
    lower = dot_t(unit, top_factor)
    for j in range(1, STEPS + 1):
        known = pad + block * j
        stacked = jnp.concatenate(thirds(coef[:, 0:known]), axis=0)

        def combine(p, first_tile, last_tile):
            at = slice(first_tile * LANES, last_tile * LANES)
            first = one(stacked, sh[p, 0:known, at])
            second = one(stacked[0 : 2 * block], sl[p, 0:known, at])
            value = first[0:block] + (first[block : 2 * block] + second[0:block])
            value = value + (first[2 * block :] + second[block:])
            vbuf[j - 1, p + 1, :, LANES + first_tile * LANES : LANES + last_tile * LANES] = value
            for tile in range(first_tile, last_tile):
                here = slice((tile - first_tile) * LANES, (tile - first_tile + 1) * LANES)
                put(sh, sl, p, known - block, tile, value[:, here])

        def combine_edges(p, carry):
            combine(p, 0, 1)
            combine(p, tiles - 1, tiles)
            return carry

        def combine_inner(p, carry):
            combine(p, 1, tiles - 1)
            return carry

        def image_inner(p, carry):
            for tile in range(1, tiles - 1):
                put(sh, sl, p, known, tile, stencil(vbuf.at[j - 1], p, tile)[0])
            return carry

        wide = known + block
        ends = (0, planes - 1)
        acc = jnp.zeros((2 * wide, 2 * block), jnp.float32)

        def gram_of(rows, rest):
            new = jnp.concatenate([rows[known:], rest[known:]], axis=0)
            return one_t(jnp.concatenate([rows, rest], axis=0), new)

        def image(p, tile):
            put(sh, sl, p, known, tile, stencil(vbuf.at[j - 1], p, tile)[0])

        def inner_gram(p, acc):
            for tile in range(1, tiles - 1):
                image(p, tile)
            at = slice(LANES, (tiles - 1) * LANES)
            return acc + gram_of(sh[p, 0:wide, at], sl[p, 0:wide, at])

        for p in ends:
            combine(p, 0, tiles)
        halo_start(has_z, lambda side: z_copy(j, side))
        for p in range(1, planes - 1):
            combine(p, 0, 1)
            combine(p, tiles - 1, tiles)
        halo_start(has_x, lambda side: x_copy(j, side))
        for p in range(1, planes - 1):
            combine(p, 1, tiles - 1)
        if planes > 2:
            acc = lax.fori_loop(1, planes - 1, inner_gram, acc, unroll=(planes - 2) // 2)
        halo_wait(has_x, lambda side: x_copy(j, side))
        lanes_of = lambda ref, p, tile: ref[p, 0:wide, tile * LANES : (tile + 1) * LANES]
        sides = [(p, tile) for p in range(1, planes - 1) for tile in (0, tiles - 1)]
        for p, tile in sides:
            image(p, tile)
        if sides:
            acc = acc + gram_of(*(
                jnp.concatenate([lanes_of(ref, p, tile) for p, tile in sides], axis=1) for ref in (sh, sl)
            ))
        halo_wait(has_z, lambda side: z_copy(j, side))
        for p in ends:
            for tile in range(tiles):
                image(p, tile)
            acc = acc + gram_of(sh[p, 0:wide, :], sl[p, 0:wide, :])
        tall = acc[0:wide, 0:block] + (acc[wide:, 0:block] + acc[0:wide, block:] + acc[wide:, block:])
        fin[0:block, 0:wide] = dot_t(unit, tall)
        early = block * (STEPS - 1)

        if j == STEPS:
            pads = jnp.zeros((early, LANES - early), jnp.float32)

            def invert_early():
                he = hbt[0:early, :]
                normal = jnp.concatenate([dot_t(he, he), pads], axis=1)
                lsq[...] = eliminate(beside(normal, early), early)
                yfirst[...] = dot(dot_t(lower, he[:, 0:block]), lsq[:, early : 2 * early])

            fin[0:block, :] = reduce_sum(gram, j - 1, fin[0:block, :], invert_early)
        else:
            fin[0:block, :] = reduce_sum(gram, j - 1, fin[0:block, :])
        wa = fin[0:block, 0:pad]
        wa_inv = dot(wa, whole_inv)
        ht = fin[0:block, pad:known]
        at = block * (j - 1)
        ebt[at : at + block, :] = wa_inv
        outside = fin[0:block, known:wide] - dot_t(wa_inv, wa)
        if j == STEPS:
            break
        fresh = outside - dot_t(ht, ht)
        lt, inv = factor(beside(full(fresh), block), block, block)
        coef[:, 0:pad] = -dot(inv, wa_inv)
        coef[:, pad:known] = -dot(inv, ht)
        coef[:, known:wide] = inv
        hbt[at : at + block, 0 : known - pad] = ht
        hbt[at : at + block, known - pad : known - pad + block] = dot_t(unit, lt)

    width = pad + block * (STEPS + 1)
    kry = block * STEPS
    he, yt0 = hbt[0:early, 0:kry], yfirst[...]
    p = lsq[:, early : 2 * early]
    cross = dot_t(ht, he)
    bent = dot(cross, p)
    schur = outside - dot_t(bent, cross)
    late_right = dot_t(lower, ht[:, 0:block]) - dot_t(yt0, cross)
    both = jnp.concatenate([schur, dot_t(unit, late_right), wide_zero[:, block:]], axis=1)
    y_late = dot_t(unit, eliminate(both, block)[:, block : 2 * block])
    y_early = yt0 - dot(y_late, bent)
    yt = jnp.concatenate([y_early, y_late], axis=1)
    back[...] = ba_inv - dot(yt, ebt[...])
    fin[...] = jnp.zeros(fin.shape, jnp.float32)
    fin[0:block, pad : pad + kry] = yt
    fin[block : 2 * block, 0:pad] = dot(y_late, wa_inv)
    fin[block : 2 * block, pad : pad + kry] = -dot(y_early, he)
    fin[block : 2 * block, pad : pad + block] = fin[block : 2 * block, pad : pad + block] + lower
    fin[block : 2 * block, pad + kry : width] = -y_late
    high, low = halves(fin[0 : 2 * block, 0:width])
    stacked = jnp.concatenate([high, low], axis=0)
    bh, bl = halves(back[...])
    bstack = jnp.concatenate([bh, bl], axis=0)

    def out_copy(kind, there):
        dst = (sol_ref, res_ref)[kind]
        return pltpu.make_async_remote_copy(
            src_ref=obuf.at[there, pl.ds(kind * block, block)], dst_ref=dst.at[core, :, part(q, ci)],
            send_sem=out_send.at[kind, there], recv_sem=out_recv.at[kind, t],
            device_id=(base + there,), device_id_type=MESH,
        )

    def out_wait(kind, there):
        dst = (sol_ref, res_ref)[kind].at[lax.rem(there, 2), :, part(gray(there // 2), ci)]
        pltpu.make_async_remote_copy(
            src_ref=dst, dst_ref=dst, send_sem=out_send.at[kind, there], recv_sem=out_recv.at[kind, there],
            device_id=(base + there,), device_id_type=MESH,
        ).wait_recv()

    def final_plane(p):
        first = one(stacked, sh[p, 0:width, :])
        both = first[0 : 2 * block] + (first[2 * block :] + one(high, sl[p, 0:width, :]))
        first = one(bstack, uh[p])
        return both[0:block] + (first[0:block] + (first[block:] + one(bh, ul[p]))), both[block:]

    def final_send(i, carry):
        there = flip(t, planes - 1 - i, bits)
        sol, res = final_plane(there)
        obuf[there, 0:block, :] = sol
        obuf[there, block:, :] = res
        for kind in range(2):
            out_copy(kind, there).start()
        return carry

    lax.fori_loop(0, planes - 1, final_send, 0)
    sol, res = final_plane(t)
    for x in range(tiles):
        sol_lines[core, :, q * tiles + x, :] = sol[:, x * LANES : (x + 1) * LANES]
        res_lines[core, :, q * tiles + x, :] = res[:, x * LANES : (x + 1) * LANES]

    for there in others:
        g, first_line = lax.rem(there, 2), gray(there // 2) * tiles
        for kind in range(2):
            out_wait(kind, there)
            landed, lines_of = (sol_ref, sol_lines, res_ref, res_lines)[2 * kind : 2 * kind + 2]
            for x in range(tiles):
                at = pl.ds(pl.multiple_of((first_line + x) * LANES, LANES), LANES)
                lines_of[g, :, first_line + x, :] = landed[g, :, at]
    for kind in range(3):
        for there in others:
            in_copy(kind, there).wait_send()
    for stage in range(STEPS + 1):
        both_sides(has_z, lambda side: z_copy(stage, side), "wait_send")
        if stage:
            both_sides(has_x, lambda side: x_copy(stage, side), "wait_send")
    reduce_drain(gram0, 0)
    for j in range(STEPS):
        reduce_drain(gram, j)
    for there in others:
        for kind in range(2):
            out_copy(kind, there).wait_send()


def split_count(n):
    out = []
    while n > 1:
        f = next(f for f in (16, 8, 4, 2, n) if n % f == 0)
        out.append(f)
        n //= f
    return out


def solution(mesh):
    n = mesh.shape["grid"]

    def on_device(right_sides, recycle, medium, shift_table, shift_index):
        block = right_sides.shape[0] // 2
        k_rows = recycle.shape[1]
        lines = right_sides.shape[2]
        cells = lines * right_sides.shape[3]
        quarters = next(q for q in (4, 2, 1) if n % (2 * q) == 0 and lines % q == 0)
        planes = 2 * quarters
        stages, stride = [], 2
        for f in split_count(n // 2):
            stages.append((f, stride))
            stride *= f
        pad = -(-k_rows // block) * block
        ci = cells // quarters
        cw = ci + 2 * LANES
        width = pad + block * (STEPS + 1)
        b = right_sides.reshape(2, block, lines, right_sides.shape[3])
        u = recycle.reshape(2, k_rows, lines, right_sides.shape[3])
        slots = sum(f for f, _ in stages)
        vmem = pl.BlockSpec(memory_space=pltpu.VMEM)
        hbm = pl.BlockSpec(memory_space=pltpu.HBM)
        shape = jax.ShapeDtypeStruct(b.shape, jnp.float32)
        f32, half = jnp.float32, jnp.bfloat16
        sems = lambda *s: pltpu.SemaphoreType.DMA(s)
        sol, res = pl.pallas_call(
            functools.partial(kernel, n, quarters, tuple(stages)),
            out_shape=(shape, shape),
            in_specs=[hbm] * 5,
            out_specs=(vmem, vmem),
            scratch_shapes=[
                pltpu.VMEM(u.shape, f32),
                pltpu.VMEM(b.shape, f32),
                pltpu.VMEM((1, cells), f32),
                pltpu.SMEM(shift_table.shape, f32),
                pltpu.SMEM(shift_index.shape, jnp.int32),
                pltpu.VMEM((2, k_rows, cells + 2 * LANES), f32),
                pltpu.VMEM((2, block, cells), f32),
                pltpu.VMEM((2, block, cells), f32),
                pltpu.VMEM((2, block, cells), f32),
                pltpu.VMEM((planes + 2, k_rows, cw), f32),
                pltpu.VMEM((STEPS, planes + 2, block, cw), f32),
                pltpu.VMEM((planes, block, ci), f32),
                pltpu.VMEM((planes, 1, ci), f32),
                pltpu.VMEM((planes, width, ci), half),
                pltpu.VMEM((planes, width, ci), half),
                pltpu.VMEM((planes, pad, ci), half),
                pltpu.VMEM((planes, pad, ci), half),
                pltpu.VMEM((planes, 2 * block, ci), f32),
                pltpu.VMEM((1, slots, k_rows, LANES), f32),
                pltpu.VMEM((STEPS, slots, block, LANES), f32),
                pltpu.VMEM((block, LANES), f32),
                pltpu.VMEM((block * STEPS, LANES), f32),
                pltpu.VMEM((block * STEPS, pad), f32),
                pltpu.VMEM((block * (STEPS - 1), LANES), f32),
                pltpu.VMEM((block, block * (STEPS - 1)), f32),
                pltpu.VMEM((pad + block, LANES), f32),
                pltpu.VMEM((pad, LANES), f32),
                pltpu.VMEM((block, pad), f32),
                sems(5),
                sems(3, planes), sems(3, planes),
                sems(STEPS + 1, 2), sems(STEPS + 1, 2),
                sems(STEPS, 2), sems(STEPS, 2),
                sems(STEPS + 1, slots), sems(STEPS + 1, slots),
                sems(2, planes), sems(2, planes),
            ],
            compiler_params=pltpu.CompilerParams(
                collective_id=0, has_side_effects=True, vmem_limit_bytes=65000000
            ),
        )(u, b, medium.reshape(1, cells), shift_table, shift_index)
        return sol.reshape(right_sides.shape), res.reshape(right_sides.shape)

    rows = P(None, "grid", None, None)
    return jax.shard_map(
        on_device,
        mesh=mesh,
        in_specs=(rows, P(None, None, "grid", None, None), P("grid", None, None), P(), P()),
        out_specs=(rows, rows),
        check_vma=False,
    )
```
